32 devices in a mesh: side: 4 (over z), rep: 8 (over y, x, core).
Axes of the slice: x: 2, y: 2, z: 4, core: 2. Of those that a mesh axis runs over, the one named last changes fastest.
Arguments:
- w_up: float32 [4, 8, 1024, 1536], P('side', None, 'rep')
- w_down: float32 [4, 8, 1536, 1024], P('side', None, None, 'rep')
- g_up: float32 [4, 8, 1024, 1536], P('side', None, 'rep')
- g_down: float32 [4, 8, 1536, 1024], P('side', None, None, 'rep')
- learn_rate: float32 [], replicated
- prompts: bfloat16 [4, 16384, 512], P('side', 'rep')
- prompt_lens: int32 [8], P('rep')
Outputs:
- output 1: float32 [4, 8, 1024, 1536], P('side', None, 'rep')
- output 2: float32 [4, 8, 1536, 1024], P('side', None, None, 'rep')
- output 3: bfloat16 [4, 16384, 512], P('side', 'rep')
All inputs are finite; a program needn't handle non-finite values.
Results may differ from the reference program's by a relative error of at most 0.01907.
Values are sent between devices in bfloat16 or wider.
A program may use at most 1 GiB of HBM per device.

```python
import jax
import jax.numpy as jnp
from jax import lax

SIDE_DEVS = 4
REP_DEVS = 8
MODEL_DIM = 1024
FFN_DIM = 3072
LAYERS = 8
TOKENS = 2048
TP_WAYS = SIDE_DEVS // 2
FF_PIECE = FFN_DIM // TP_WAYS
D_PIECE = MODEL_DIM // TP_WAYS


def draw_lens(len_key):
    key_a, key_b = jax.random.split(len_key)
    low_len = max(1, TOKENS // 32)
    base_lens = jax.random.randint(key_a, (REP_DEVS,), low_len, TOKENS + 1, jnp.int32)
    full_slot = jax.random.randint(key_b, (), 0, REP_DEVS, jnp.int32)
    return jnp.where(jnp.arange(REP_DEVS) == full_slot, TOKENS, base_lens).astype(jnp.int32)


def setup_inputs(seed: int = 0) -> dict:
    sub_keys = jax.random.split(jax.random.key(seed), 7)
    up_shape = (TP_WAYS, LAYERS, MODEL_DIM, FF_PIECE)
    down_shape = (TP_WAYS, LAYERS, FF_PIECE, MODEL_DIM)
    up_scale = MODEL_DIM ** -0.5
    down_scale = 0.7 * FFN_DIM ** -0.5
    w_up = jax.random.normal(sub_keys[0], up_shape, jnp.float32) * up_scale
    w_down = jax.random.normal(sub_keys[1], down_shape, jnp.float32) * down_scale
    g_up = jax.random.normal(sub_keys[2], up_shape, jnp.float32) * up_scale
    g_down = jax.random.normal(sub_keys[3], down_shape, jnp.float32) * down_scale
    learn_rate = jax.random.uniform(sub_keys[4], (), jnp.float32, 0.02, 0.25)
    gen_rows = jax.random.normal(sub_keys[5], (TP_WAYS, REP_DEVS * TOKENS, D_PIECE), jnp.float32)
    prompts = jnp.concatenate([jnp.zeros_like(gen_rows), gen_rows], axis=0).astype(jnp.bfloat16)
    return {
        "w_up": jnp.concatenate([w_up, jnp.zeros_like(w_up)], axis=0),
        "w_down": jnp.concatenate([w_down, jnp.zeros_like(w_down)], axis=0),
        "g_up": jnp.concatenate([g_up, jnp.zeros_like(g_up)], axis=0),
        "g_down": jnp.concatenate([g_down, jnp.zeros_like(g_down)], axis=0),
        "learn_rate": learn_rate,
        "prompts": prompts,
        "prompt_lens": draw_lens(sub_keys[6]),
    }


def reference(w_up, w_down, g_up, g_down, learn_rate, prompts, prompt_lens):
    new_up = w_up - learn_rate * g_up
    new_down = w_down - learn_rate * g_down
    up_bf = new_up[:TP_WAYS].astype(jnp.bfloat16)
    down_bf = new_down[:TP_WAYS].astype(jnp.bfloat16)
    up_full = jnp.transpose(up_bf, (1, 2, 0, 3)).reshape(LAYERS, MODEL_DIM, FFN_DIM)
    down_full = jnp.transpose(down_bf, (1, 0, 2, 3)).reshape(LAYERS, FFN_DIM, MODEL_DIM)
    x_full = jnp.transpose(prompts[TP_WAYS:], (1, 0, 2)).reshape(REP_DEVS, TOKENS, MODEL_DIM)

    def layer_step(h_rows, layer_w):
        up_layer, down_layer = layer_w
        pre_act = jnp.dot(h_rows, up_layer, preferred_element_type=jnp.float32)
        act_bf = jax.nn.gelu(pre_act, approximate=True).astype(jnp.bfloat16)
        part_sum = jnp.dot(act_bf, down_layer, preferred_element_type=jnp.float32)
        return (h_rows.astype(jnp.float32) + part_sum).astype(jnp.bfloat16), None

    def one_replica(replica_in):
        row_block, length = replica_in
        h_rows, _ = lax.scan(layer_step, row_block, (up_full, down_full))
        keep_mask = jnp.arange(TOKENS)[:, None] < length
        return jnp.where(keep_mask, h_rows, jnp.zeros_like(h_rows))

    y_full = lax.map(one_replica, (x_full, prompt_lens))
    y_gen = jnp.transpose(y_full.reshape(REP_DEVS * TOKENS, TP_WAYS, D_PIECE), (1, 0, 2))
    outputs = jnp.concatenate([jnp.zeros_like(y_gen), y_gen], axis=0)
    return new_up, new_down, outputs
```

```python
import functools

import jax
import jax.numpy as jnp
from jax import lax
from jax.experimental import pallas as pl
from jax.experimental.pallas import tpu as pltpu
from jax.sharding import PartitionSpec as P

MESH = pl.DeviceIdType.MESH
PLANES = 4
REPS = 8


def _gelu(z):
    inner = 0.7978845608028654 * (z + 0.044715 * (z * z * z))
    return z * (0.5 * (1.0 + jnp.tanh(inner)))


def _pipeline_kernel(
    upb, dnb, x_ref, y_ref,
    wu, wd, hin, hout, mid, act,
    z_recv, z_send, x_recv, x_send, y_recv, y_send, d_recv, d_send, s_recv, s_send,
    in_recv, in_send, h_recv, h_send, out_recv, out_send, out_loc,
    *, chunk, tile_n, tile_m,
):
    z = lax.axis_index("side")
    r = lax.axis_index("rep")
    core = r % 2
    xpos = (r // 2) % 2
    ypos = r // 4
    r_x = r + 2 - 4 * xpos
    r_y = r + 4 - 8 * ypos
    r_d = r_x + 4 - 8 * ypos
    r_s = r + 1 - 2 * core

    width = upb.shape[1]
    ff = upb.shape[2]
    tokens, d_half = x_ref.shape
    n_chunks = tokens // chunk
    first_rank = jnp.minimum(z, 1)

    def dev(zz, rr):
        return (zz, rr)

    barrier = pltpu.get_barrier_semaphore()
    for step in range(1, PLANES):
        pl.semaphore_signal(barrier, inc=1, device_id=dev((z + step) % PLANES, r), device_id_type=MESH)
    for rr in (r_x, r_y, r_s):
        pl.semaphore_signal(barrier, inc=1, device_id=dev(z, rr), device_id_type=MESH)
    pl.semaphore_wait(barrier, PLANES + 2)

    def remote(src, dst, send, recv, to):
        return pltpu.make_async_remote_copy(
            src_ref=src, dst_ref=dst, send_sem=send, recv_sem=recv, device_id=to, device_id_type=MESH)

    def piece(jk, rank, rr):
        j, k = jk // 2, jk % 2
        off = pl.multiple_of(rr * width, width)
        if isinstance(rank, int):
            hid = pl.ds(rank * ff, ff)
        else:
            hid = pl.ds(pl.multiple_of(rank * ff, ff), ff)
        if k == 0:
            return wu.at[j, pl.ds(off, width), hid]
        return wd.at[j, hid, pl.ds(off, width)]

    def shard(jk, plane):
        src = upb if jk % 2 == 0 else dnb
        return src.at[2 * plane + jk // 2]

    def prompt_copy(i):
        rows = pl.ds(pl.multiple_of(i * chunk, chunk), chunk)
        half = jnp.maximum(z - 2, 0)
        cols = pl.ds(pl.multiple_of(half * d_half, d_half), d_half)
        return remote(x_ref.at[rows, :], hin.at[rows, cols], in_send.at[i],
                      in_recv.at[half * n_chunks + i], dev(0, r))

    @pl.when(z >= 2)
    def _():
        def body(i, carry):
            prompt_copy(i).start()
            return carry
        lax.fori_loop(0, n_chunks, body, 0)

    def weight_copy(rank, plane, jk):
        e = jk if rank == min(plane, 1) else jk + 4
        if plane == rank:
            return pltpu.make_async_copy(shard(jk, plane), piece(jk, rank, r), z_recv.at[e])
        return remote(shard(jk, plane), piece(jk, rank, r), z_send.at[plane * 4 + jk],
                      z_recv.at[e], dev(plane, r))

    for rank in range(2):
        @pl.when(z == rank)
        def _():
            for plane in [rank] + [p for p in range(PLANES) if p != rank]:
                for jk in range(4):
                    weight_copy(rank, plane, jk).start()

    def rank_of(e):
        return first_rank if e < 4 else 1 - first_rank

    def spread(e, kind):
        jk = e % 4
        own = piece(jk, rank_of(e), r)
        if kind == "x":
            return remote(own, own, x_send.at[e], x_recv.at[e], dev(z, r_x))
        return remote(own, own, y_send.at[e], y_recv.at[e], dev(z, r_y))

    def relay(e):
        jk = e % 4
        if jk % 2 == 0:
            ref, to = piece(jk, rank_of(e), r_x), r_y
        else:
            ref, to = piece(jk, rank_of(e), r_y), r_x
        return remote(ref, ref, d_send.at[e], d_recv.at[e], dev(z, to))

    def to_sibling(e, q):
        ref = piece(e % 4, rank_of(e), (r, r_x, r_y, r_d)[q])
        return remote(ref, ref, s_send.at[q * 8 + e], s_recv.at[q * 8 + e], dev(z, r_s))

    def from_sibling(e, q):
        flip = 1 - 2 * core
        ref = piece(e % 4, rank_of(e), (r, r_x, r_y, r_d)[q] + flip)
        return remote(ref, ref, s_send.at[q * 8 + e], s_recv.at[q * 8 + e], dev(z, r_s))

    def landed(ref, sem):
        remote(ref, ref, sem, sem, dev(z, r_s)).wait_recv()

    for i in range(8 + 4):
        if i < 8:
            landed(piece(i % 4, rank_of(i), r), z_recv.at[i])
            spread(i, "x").start()
            spread(i, "y").start()
            to_sibling(i, 0).start()
        if 0 <= i - 2 < 8:
            e = i - 2
            landed(piece(e % 4, rank_of(e), r_x), x_recv.at[e])
            if e % 2 == 0:
                relay(e).start()
            landed(piece(e % 4, rank_of(e), r_y), y_recv.at[e])
            if e % 2 == 1:
                relay(e).start()
            to_sibling(e, 1).start()
            to_sibling(e, 2).start()
        if 0 <= i - 4 < 8:
            e = i - 4
            landed(piece(e % 4, rank_of(e), r_d), d_recv.at[e])
            to_sibling(e, 3).start()
    for e in range(8):
        for q in range(4):
            from_sibling(e, q).wait_recv()

    hidden = wu.shape[2]
    model = wu.shape[1]

    def hop_copy(i):
        rows = pl.ds(pl.multiple_of(i * chunk, chunk), chunk)
        return remote(hout.at[rows, :], hin.at[rows, :], h_send.at[i], h_recv.at[i],
                      dev(jnp.minimum(z + 1, PLANES - 1), r))

    def out_remote(i):
        rows = pl.ds(pl.multiple_of(i * chunk, chunk), chunk)
        return remote(hout.at[rows, pl.ds(0, d_half)], y_ref.at[rows, :], out_send.at[i], out_recv.at[i], dev(2, r))

    def out_local(i):
        rows = pl.ds(pl.multiple_of(i * chunk, chunk), chunk)
        return pltpu.make_async_copy(hout.at[rows, pl.ds(d_half, d_half)], y_ref.at[rows, :], out_loc.at[i])

    def layer(j, src, src_rows, dst, dst_rows):
        for n in range(hidden // tile_n):
            cols = pl.ds(n * tile_n, tile_n)
            pre = jnp.dot(src[src_rows, :], wu[j, :, cols], preferred_element_type=jnp.float32)
            act[:, cols] = _gelu(pre).astype(jnp.bfloat16)
        for m in range(model // tile_m):
            cols = pl.ds(m * tile_m, tile_m)
            part = jnp.dot(act[...], wd[j, :, cols], preferred_element_type=jnp.float32)
            dst[dst_rows, cols] = (src[src_rows, cols].astype(jnp.float32) + part).astype(jnp.bfloat16)

    def chunk_step(i, carry):
        rows = pl.ds(pl.multiple_of(i * chunk, chunk), chunk)

        @pl.when(z == 0)
        def _():
            for half in range(2):
                landed(hin.at[rows, pl.ds(half * d_half, d_half)], in_recv.at[half * n_chunks + i])

        @pl.when(z > 0)
        def _():
            landed(hin.at[rows, :], h_recv.at[i])

        layer(0, hin, rows, mid, pl.ds(0, chunk))
        layer(1, mid, pl.ds(0, chunk), hout, rows)

        @pl.when(z < PLANES - 1)
        def _():
            hop_copy(i).start()

        @pl.when(z == PLANES - 1)
        def _():
            out_remote(i).start()
            out_local(i).start()

        return carry

    lax.fori_loop(0, n_chunks, chunk_step, 0)

    def drain(fn):
        def body(i, carry):
            fn(i)
            return carry
        lax.fori_loop(0, n_chunks, body, 0)

    @pl.when(z >= 2)
    def _():
        drain(lambda i: prompt_copy(i).wait_send())

    for rank in range(2):
        @pl.when(z == rank)
        def _():
            for plane in range(PLANES):
                if plane != rank:
                    for jk in range(4):
                        weight_copy(rank, plane, jk).wait_send()

    for e in range(8):
        spread(e, "x").wait_send()
        spread(e, "y").wait_send()
        relay(e).wait_send()
        for q in range(4):
            to_sibling(e, q).wait_send()

    @pl.when(z < PLANES - 1)
    def _():
        drain(lambda i: hop_copy(i).wait_send())

    @pl.when(z == PLANES - 1)
    def _():
        drain(lambda i: out_remote(i).wait_send())
        drain(lambda i: out_local(i).wait())

    @pl.when(z == 2)
    def _():
        drain(lambda i: out_remote(i).wait_recv())


def solution(mesh):
    side_devs = mesh.shape["side"]
    tp_ways = side_devs // 2
    up_spec = P("side", None, "rep", None)
    down_spec = P("side", None, None, "rep")
    act_spec = P("side", "rep", None)

    def device_step(w_up, w_down, g_up, g_down, learn_rate, prompts, prompt_lens):
        new_up = w_up - learn_rate * g_up
        new_down = w_down - learn_rate * g_down
        upb = new_up[0].astype(jnp.bfloat16)
        dnb = new_down[0].astype(jnp.bfloat16)
        layers, width, ff = upb.shape
        tokens, d_half = prompts.shape[1:]
        model, hidden = width * REPS, ff * tp_ways
        chunk = min(256, tokens // 4)
        n_chunks = tokens // chunk
        dma = pltpu.SemaphoreType.DMA
        hbm = pl.BlockSpec(memory_space=pltpu.HBM)
        y = pl.pallas_call(
            functools.partial(_pipeline_kernel, chunk=chunk, tile_n=min(512, ff), tile_m=min(512, d_half)),
            out_shape=jax.ShapeDtypeStruct((tokens, d_half), jnp.bfloat16),
            in_specs=[hbm, hbm, hbm],
            out_specs=hbm,
            scratch_shapes=[
                pltpu.VMEM((2, model, hidden), jnp.bfloat16),
                pltpu.VMEM((2, hidden, model), jnp.bfloat16),
                pltpu.VMEM((tokens, model), jnp.bfloat16),
                pltpu.VMEM((tokens, model), jnp.bfloat16),
                pltpu.VMEM((chunk, model), jnp.bfloat16),
                pltpu.VMEM((chunk, hidden), jnp.bfloat16),
                dma((8,)), dma((16,)), dma((8,)), dma((8,)), dma((8,)), dma((8,)),
                dma((8,)), dma((8,)), dma((32,)), dma((32,)),
                dma((2 * n_chunks,)), dma((n_chunks,)), dma((n_chunks,)), dma((n_chunks,)),
                dma((n_chunks,)), dma((n_chunks,)), dma((n_chunks,)),
            ],
            compiler_params=pltpu.CompilerParams(
                collective_id=0, has_side_effects=True, vmem_limit_bytes=60 * 1024 * 1024),
            name="layer_pipeline",
        )(upb, dnb, prompts[0])
        side_idx = lax.axis_index("side")
        keep = (jnp.arange(tokens)[:, None] < prompt_lens[0]) & (side_idx >= tp_ways)
        out_block = jnp.where(keep, y, jnp.zeros_like(y))
        return new_up, new_down, out_block[None]

    return jax.shard_map(
        device_step,
        mesh=mesh,
        in_specs=(up_spec, down_spec, up_spec, down_spec, P(), act_spec, P("rep")),
        out_specs=(up_spec, down_spec, act_spec),
        check_vma=False,
    )
```

```python
import functools

import jax
import jax.numpy as jnp
from jax import lax
from jax.experimental import pallas as pl
from jax.experimental.pallas import tpu as pltpu
from jax.sharding import PartitionSpec as P

MESH = pl.DeviceIdType.MESH
PLANES = 4
REPS = 8
UNITS = ((0, 0), (0, 1), (0, 2), (1, 0), (0, 3), (1, 1), (1, 2), (1, 3))


def _gelu(z):
    inner = 0.7978845608028654 * (z + 0.044715 * (z * z * z))
    return z * (0.5 * (1.0 + jnp.tanh(inner)))


def _pipeline_kernel(
    upb, dnb, x_ref, y_ref,
    wu, wd, hin, hout, mid, act,
    z_recv, z_send, x_recv, x_send, y_recv, y_send, d_recv, d_send, s_recv, s_send,
    in_recv, in_send, h_recv, h_send, out_recv, out_send, out_loc,
    *, chunk, tile_n, tile_m,
):
    z = lax.axis_index("side")
    r = lax.axis_index("rep")
    core = r % 2
    xpos = (r // 2) % 2
    ypos = r // 4
    r_x = r + 2 - 4 * xpos
    r_y = r + 4 - 8 * ypos
    r_d = r_x + 4 - 8 * ypos
    r_s = r + 1 - 2 * core

    width = upb.shape[1]
    ff = upb.shape[2]
    tokens, d_half = x_ref.shape
    first_rank = jnp.minimum(z, 1)
    n_big = tokens // chunk - 1
    small = chunk // 2
    n_chunks = n_big + 2

    def dev(zz, rr):
        return (zz, rr)

    barrier = pltpu.get_barrier_semaphore()
    scope = jax.named_scope
    for step in range(1, PLANES):
        pl.semaphore_signal(barrier, inc=1, device_id=dev((z + step) % PLANES, r), device_id_type=MESH)
    for rr in (r_x, r_y, r_s):
        pl.semaphore_signal(barrier, inc=1, device_id=dev(z, rr), device_id_type=MESH)
    with scope("entry"):
        pl.semaphore_wait(barrier, PLANES + 2)

    def remote(src, dst, send, recv, to):
        return pltpu.make_async_remote_copy(
            src_ref=src, dst_ref=dst, send_sem=send, recv_sem=recv, device_id=to, device_id_type=MESH)

    def piece(jk, rank, rr):
        j, k = jk // 2, jk % 2
        off = pl.multiple_of(rr * width, width)
        if isinstance(rank, int):
            hid = pl.ds(rank * ff, ff)
        else:
            hid = pl.ds(pl.multiple_of(rank * ff, ff), ff)
        if k == 0:
            return wu.at[j, pl.ds(off, width), hid]
        return wd.at[j, hid, pl.ds(off, width)]

    def shard(jk, plane):
        src = upb if jk % 2 == 0 else dnb
        return src.at[2 * plane + jk // 2]

    def big(i):
        return pl.ds(pl.multiple_of(i * chunk, chunk), chunk)

    def tail(i):
        return pl.ds(n_big * chunk + (i - n_big) * small, small)

    def prompt_copy(i, rows):
        half = jnp.maximum(z - 2, 0)
        cols = pl.ds(pl.multiple_of(half * d_half, d_half), d_half)
        return remote(x_ref.at[rows, :], hin.at[rows, cols], in_send.at[i],
                      in_recv.at[half * n_chunks + i], dev(0, r))

    def each_chunk(fn):
        def body(i, carry):
            fn(i, big(i))
            return carry
        lax.fori_loop(0, n_big, body, 0)
        for i in range(n_big, n_chunks):
            fn(i, tail(i))

    def weight_copy(rank, plane, jk):
        e = UNITS.index((0 if rank == min(plane, 1) else 1, jk))
        if plane == rank:
            return pltpu.make_async_copy(shard(jk, plane), piece(jk, rank, r), z_recv.at[e])
        return remote(shard(jk, plane), piece(jk, rank, r), z_send.at[plane * 4 + jk],
                      z_recv.at[e], dev(plane, r))

    for rank in range(2):
        @pl.when(z == rank)
        def _():
            order = [(rank, jk) for jk in range(4)] + [(1 - rank, jk) for jk in range(4)]
            order += [(plane, jk) for jk in range(4) for plane in (2, 3)]
            for plane, jk in order:
                weight_copy(rank, plane, jk).start()

    def unit(e, rr):
        late, jk = UNITS[e]
        return piece(jk, 1 - first_rank if late else first_rank, rr)

    def spread(e, kind):
        own = unit(e, r)
        if kind == "x":
            return remote(own, own, x_send.at[e], x_recv.at[e], dev(z, r_x))
        return remote(own, own, y_send.at[e], y_recv.at[e], dev(z, r_y))

    def relay(e):
        if UNITS[e][1] % 2 == 0:
            ref, to = unit(e, r_x), r_y
        else:
            ref, to = unit(e, r_y), r_x
        return remote(ref, ref, d_send.at[e], d_recv.at[e], dev(z, to))

    def to_sibling(e, q):
        ref = unit(e, (r, r_x, r_y, r_d)[q])
        return remote(ref, ref, s_send.at[q * 8 + e], s_recv.at[q * 8 + e], dev(z, r_s))

    def landed(ref, sem):
        remote(ref, ref, sem, sem, dev(z, r_s)).wait_recv()

    def from_sibling(e, q):
        landed(unit(e, (r, r_x, r_y, r_d)[q] + 1 - 2 * core), s_recv.at[q * 8 + e])

    for i in range(8 + 4):
        if 0 <= i - 4:
            e = i - 4
            with scope(f"dw{e}"):
                landed(unit(e, r_d), d_recv.at[e])
            to_sibling(e, 3).start()
        if 0 <= i - 2 < 8:
            e = i - 2
            with scope(f"xw{e}"):
                landed(unit(e, r_x), x_recv.at[e])
                landed(unit(e, r_y), y_recv.at[e])
            relay(e).start()
            to_sibling(e, 1).start()
            to_sibling(e, 2).start()
        if i < 8:
            with scope(f"zw{i}"):
                landed(unit(i, r), z_recv.at[i])
            spread(i, "x").start()
            spread(i, "y").start()
            to_sibling(i, 0).start()
        if i == 1:
            @pl.when(z >= 2)
            def _():
                each_chunk(lambda c, rows: prompt_copy(c, rows).start())
    with scope("sib"):
        for e in range(8):
            for q in range(4):
                from_sibling(e, q)

    hidden = wu.shape[2]
    model = wu.shape[1]

    def hop_copy(i, rows):
        return remote(hout.at[rows, :], hin.at[rows, :], h_send.at[i], h_recv.at[i],
                      dev(jnp.minimum(z + 1, PLANES - 1), r))

    def out_remote(i, rows):
        return remote(hout.at[rows, pl.ds(0, d_half)], y_ref.at[rows, :], out_send.at[i], out_recv.at[i], dev(2, r))

    def out_local(i, rows):
        return pltpu.make_async_copy(hout.at[rows, pl.ds(d_half, d_half)], y_ref.at[rows, :], out_loc.at[i])

    def layer(j, src, src_rows, dst, dst_rows, size):
        for n in range(hidden // tile_n):
            cols = pl.ds(n * tile_n, tile_n)
            pre = jnp.dot(src[src_rows, :], wu[j, :, cols], preferred_element_type=jnp.float32)
            act[:size, cols] = _gelu(pre).astype(jnp.bfloat16)
        for m in range(model // tile_m):
            cols = pl.ds(m * tile_m, tile_m)
            part = jnp.dot(act[:size, :], wd[j, :, cols], preferred_element_type=jnp.float32)
            dst[dst_rows, cols] = (src[src_rows, cols].astype(jnp.float32) + part).astype(jnp.bfloat16)

    def chunk_step(i, rows):
        size = rows.size

        @pl.when(z == 0)
        def _():
            for half in range(2):
                landed(hin.at[rows, pl.ds(half * d_half, d_half)], in_recv.at[half * n_chunks + i])

        @pl.when(z > 0)
        def _():
            landed(hin.at[rows, :], h_recv.at[i])

        with scope("layers"):
            layer(0, hin, rows, mid, pl.ds(0, size), size)
            layer(1, mid, pl.ds(0, size), hout, rows, size)

        @pl.when(z < PLANES - 1)
        def _():
            hop_copy(i, rows).start()

        @pl.when(z == PLANES - 1)
        def _():
            out_remote(i, rows).start()
            out_local(i, rows).start()

    def big_step(i, carry):
        chunk_step(i, big(i))
        return carry

    def small_step(i, carry):
        chunk_step(i, pl.ds(pl.multiple_of(n_big * chunk + (i - n_big) * small, small), small))
        return carry

    lax.fori_loop(0, n_big, big_step, 0)
    lax.fori_loop(n_big, n_chunks, small_step, 0)

    @pl.when(z >= 2)
    def _():
        each_chunk(lambda i, rows: prompt_copy(i, rows).wait_send())

    for rank in range(2):
        @pl.when(z == rank)
        def _():
            for plane in range(PLANES):
                if plane != rank:
                    for jk in range(4):
                        weight_copy(rank, plane, jk).wait_send()

    for e in range(8):
        spread(e, "x").wait_send()
        spread(e, "y").wait_send()
        relay(e).wait_send()
        for q in range(4):
            to_sibling(e, q).wait_send()

    @pl.when(z < PLANES - 1)
    def _():
        each_chunk(lambda i, rows: hop_copy(i, rows).wait_send())

    @pl.when(z == PLANES - 1)
    def _():
        each_chunk(lambda i, rows: out_remote(i, rows).wait_send())
        each_chunk(lambda i, rows: out_local(i, rows).wait())

    @pl.when(z == 2)
    def _():
        each_chunk(lambda i, rows: out_remote(i, rows).wait_recv())


def solution(mesh):
    side_devs = mesh.shape["side"]
    tp_ways = side_devs // 2
    up_spec = P("side", None, "rep", None)
    down_spec = P("side", None, None, "rep")
    act_spec = P("side", "rep", None)

    def device_step(w_up, w_down, g_up, g_down, learn_rate, prompts, prompt_lens):
        new_up = w_up - learn_rate * g_up
        new_down = w_down - learn_rate * g_down
        upb = new_up[0].astype(jnp.bfloat16)
        dnb = new_down[0].astype(jnp.bfloat16)
        layers, width, ff = upb.shape
        tokens, d_half = prompts.shape[1:]
        model, hidden = width * REPS, ff * tp_ways
        chunk = min(256, tokens // 4)
        n_chunks = tokens // chunk + 1
        dma = pltpu.SemaphoreType.DMA
        hbm = pl.BlockSpec(memory_space=pltpu.HBM)
        y = pl.pallas_call(
            functools.partial(_pipeline_kernel, chunk=chunk, tile_n=min(512, ff), tile_m=min(512, d_half)),
            out_shape=jax.ShapeDtypeStruct((tokens, d_half), jnp.bfloat16),
            in_specs=[hbm, hbm, hbm],
            out_specs=hbm,
            scratch_shapes=[
                pltpu.VMEM((2, model, hidden), jnp.bfloat16),
                pltpu.VMEM((2, hidden, model), jnp.bfloat16),
                pltpu.VMEM((tokens, model), jnp.bfloat16),
                pltpu.VMEM((tokens, model), jnp.bfloat16),
                pltpu.VMEM((chunk, model), jnp.bfloat16),
                pltpu.VMEM((chunk, hidden), jnp.bfloat16),
                dma((8,)), dma((16,)), dma((8,)), dma((8,)), dma((8,)), dma((8,)),
                dma((8,)), dma((8,)), dma((32,)), dma((32,)),
                dma((2 * n_chunks,)), dma((n_chunks,)), dma((n_chunks,)), dma((n_chunks,)),
                dma((n_chunks,)), dma((n_chunks,)), dma((n_chunks,)),
            ],
            compiler_params=pltpu.CompilerParams(
                collective_id=0, has_side_effects=True, vmem_limit_bytes=60 * 1024 * 1024),
            name="layer_pipeline",
        )(upb, dnb, prompts[0])
        side_idx = lax.axis_index("side")
        keep = (jnp.arange(tokens)[:, None] < prompt_lens[0]) & (side_idx >= tp_ways)
        out_block = jnp.where(keep, y, jnp.zeros_like(y))
        return new_up, new_down, out_block[None]

    return jax.shard_map(
        device_step,
        mesh=mesh,
        in_specs=(up_spec, down_spec, up_spec, down_spec, P(), act_spec, P("rep")),
        out_specs=(up_spec, down_spec, act_spec),
        check_vma=False,
    )
```

```python
import functools

import jax
import jax.numpy as jnp
from jax import lax
from jax.experimental import pallas as pl
from jax.experimental.pallas import tpu as pltpu
from jax.sharding import PartitionSpec as P

MESH = pl.DeviceIdType.MESH
PLANES = 4
REPS = 8
UNITS = ((0, 0), (0, 1), (1, 0), (1, 1), (1, 2), (1, 3), (0, 2), (0, 3))


def _gelu(z):
    inner = 0.7978845608028654 * (z + 0.044715 * (z * z * z))
    return z * (0.5 * (1.0 + jnp.tanh(inner)))


def _pipeline_kernel(
    upb, dnb, x_ref, y_ref,
    wu, wd, hin, hout, mid, act,
    z_recv, z_send, x_recv, x_send, y_recv, y_send, d_recv, d_send, s_recv, s_send,
    in_recv, in_send, h_recv, h_send, out_recv, out_send, out_loc,
    *, chunk, tile_n, tile_m,
):
    z = lax.axis_index("side")
    r = lax.axis_index("rep")
    core = r % 2
    xpos = (r // 2) % 2
    ypos = r // 4
    r_x = r + 2 - 4 * xpos
    r_y = r + 4 - 8 * ypos
    r_d = r_x + 4 - 8 * ypos
    r_s = r + 1 - 2 * core

    width = upb.shape[1]
    ff = upb.shape[2]
    tokens, d_half = x_ref.shape
    first_rank = jnp.minimum(z, 1)
    n_big = tokens // chunk - 1
    last = n_big * chunk
    tails = ((last, chunk // 2), (last + chunk // 2, chunk // 4), (last + 3 * chunk // 4, chunk // 4))
    n_chunks = n_big + len(tails)

    def dev(zz, rr):
        return (zz, rr)

    barrier = pltpu.get_barrier_semaphore()
    scope = jax.named_scope
    for step in range(1, PLANES):
        pl.semaphore_signal(barrier, inc=1, device_id=dev((z + step) % PLANES, r), device_id_type=MESH)
    for rr in (r_x, r_y, r_s):
        pl.semaphore_signal(barrier, inc=1, device_id=dev(z, rr), device_id_type=MESH)
    with scope("entry"):
        pl.semaphore_wait(barrier, PLANES + 2)

    def remote(src, dst, send, recv, to):
        return pltpu.make_async_remote_copy(
            src_ref=src, dst_ref=dst, send_sem=send, recv_sem=recv, device_id=to, device_id_type=MESH)

    def piece(jk, rank, rr):
        j, k = jk // 2, jk % 2
        off = pl.multiple_of(rr * width, width)
        if isinstance(rank, int):
            hid = pl.ds(rank * ff, ff)
        else:
            hid = pl.ds(pl.multiple_of(rank * ff, ff), ff)
        if k == 0:
            return wu.at[j, pl.ds(off, width), hid]
        return wd.at[j, hid, pl.ds(off, width)]

    def shard(jk, plane):
        src = upb if jk % 2 == 0 else dnb
        return src.at[2 * plane + jk // 2]

    def big(i):
        return pl.ds(pl.multiple_of(i * chunk, chunk), chunk)

    def tail(i):
        return pl.ds(*tails[i - n_big])

    def prompt_copy(i, rows):
        half = jnp.maximum(z - 2, 0)
        cols = pl.ds(pl.multiple_of(half * d_half, d_half), d_half)
        return remote(x_ref.at[rows, :], hin.at[rows, cols], in_send.at[i],
                      in_recv.at[half * n_chunks + i], dev(0, r))

    def each_chunk(fn):
        def body(i, carry):
            fn(i, big(i))
            return carry
        lax.fori_loop(0, n_big, body, 0)
        for i in range(n_big, n_chunks):
            fn(i, tail(i))

    def weight_copy(rank, plane, jk):
        e = UNITS.index((0 if rank == min(plane, 1) else 1, jk))
        if plane == rank:
            return pltpu.make_async_copy(shard(jk, plane), piece(jk, rank, r), z_recv.at[e])
        return remote(shard(jk, plane), piece(jk, rank, r), z_send.at[plane * 4 + jk],
                      z_recv.at[e], dev(plane, r))

    for rank in range(2):
        @pl.when(z == rank)
        def _():
            order = [(rank, jk) for jk in range(4)] + [(1 - rank, jk) for jk in range(4)]
            order += [(plane, jk) for jk in range(4) for plane in (2, 3)]
            for plane, jk in order:
                weight_copy(rank, plane, jk).start()

    def unit(e, rr):
        late, jk = UNITS[e]
        return piece(jk, 1 - first_rank if late else first_rank, rr)

    def spread(e, kind):
        own = unit(e, r)
        if kind == "x":
            return remote(own, own, x_send.at[e], x_recv.at[e], dev(z, r_x))
        return remote(own, own, y_send.at[e], y_recv.at[e], dev(z, r_y))

    def relay(e):
        if UNITS[e][1] % 2 == 0:
            ref, to = unit(e, r_x), r_y
        else:
            ref, to = unit(e, r_y), r_x
        return remote(ref, ref, d_send.at[e], d_recv.at[e], dev(z, to))

    def to_sibling(e, q):
        ref = unit(e, (r, r_x, r_y, r_d)[q])
        return remote(ref, ref, s_send.at[q * 8 + e], s_recv.at[q * 8 + e], dev(z, r_s))

    def landed(ref, sem):
        remote(ref, ref, sem, sem, dev(z, r_s)).wait_recv()

    def from_sibling(e, q):
        landed(unit(e, (r, r_x, r_y, r_d)[q] + 1 - 2 * core), s_recv.at[q * 8 + e])

    for i in range(8 + 4):
        if 0 <= i - 4:
            e = i - 4
            with scope(f"dw{e}"):
                landed(unit(e, r_d), d_recv.at[e])
            to_sibling(e, 3).start()
        if 0 <= i - 2 < 8:
            e = i - 2
            with scope(f"xw{e}"):
                landed(unit(e, r_x), x_recv.at[e])
                landed(unit(e, r_y), y_recv.at[e])
            relay(e).start()
            to_sibling(e, 1).start()
            to_sibling(e, 2).start()
        if i < 8:
            with scope(f"zw{i}"):
                landed(unit(i, r), z_recv.at[i])
            spread(i, "x").start()
            spread(i, "y").start()
            to_sibling(i, 0).start()
        if i == 2:
            @pl.when(z >= 2)
            def _():
                each_chunk(lambda c, rows: prompt_copy(c, rows).start())
    with scope("sib"):
        for e in range(8):
            for q in range(4):
                from_sibling(e, q)

    hidden = wu.shape[2]
    model = wu.shape[1]

    def hop_copy(i, rows):
        return remote(hout.at[rows, :], hin.at[rows, :], h_send.at[i], h_recv.at[i],
                      dev(jnp.minimum(z + 1, PLANES - 1), r))

    def out_remote(i, rows):
        return remote(hout.at[rows, pl.ds(0, d_half)], y_ref.at[rows, :], out_send.at[i], out_recv.at[i], dev(2, r))

    def out_local(i, rows):
        return pltpu.make_async_copy(hout.at[rows, pl.ds(d_half, d_half)], y_ref.at[rows, :], out_loc.at[i])

    def layer(j, src, src_rows, dst, dst_rows, size):
        for n in range(hidden // tile_n):
            cols = pl.ds(n * tile_n, tile_n)
            pre = jnp.dot(src[src_rows, :], wu[j, :, cols], preferred_element_type=jnp.float32)
            act[:size, cols] = _gelu(pre).astype(jnp.bfloat16)
        for m in range(model // tile_m):
            cols = pl.ds(m * tile_m, tile_m)
            part = jnp.dot(act[:size, :], wd[j, :, cols], preferred_element_type=jnp.float32)
            dst[dst_rows, cols] = (src[src_rows, cols].astype(jnp.float32) + part).astype(jnp.bfloat16)

    def chunk_step(i, rows):
        size = rows.size

        @pl.when(z == 0)
        def _():
            for half in range(2):
                landed(hin.at[rows, pl.ds(half * d_half, d_half)], in_recv.at[half * n_chunks + i])

        @pl.when(z > 0)
        def _():
            landed(hin.at[rows, :], h_recv.at[i])

        with scope("layers"):
            layer(0, hin, rows, mid, pl.ds(0, size), size)
            layer(1, mid, pl.ds(0, size), hout, rows, size)

        @pl.when(z < PLANES - 1)
        def _():
            hop_copy(i, rows).start()

        @pl.when(z == PLANES - 1)
        def _():
            out_remote(i, rows).start()
            out_local(i, rows).start()

    def big_step(i, carry):
        chunk_step(i, big(i))
        return carry

    def last_step(i, carry):
        size = chunk // 4
        chunk_step(i, pl.ds(pl.multiple_of(tokens - (n_chunks - i) * size, size), size))
        return carry

    lax.fori_loop(0, n_big, big_step, 0)
    chunk_step(n_big, tail(n_big))
    lax.fori_loop(n_big + 1, n_chunks, last_step, 0)

    @pl.when(z >= 2)
    def _():
        each_chunk(lambda i, rows: prompt_copy(i, rows).wait_send())

    for rank in range(2):
        @pl.when(z == rank)
        def _():
            for plane in range(PLANES):
                if plane != rank:
                    for jk in range(4):
                        weight_copy(rank, plane, jk).wait_send()

    for e in range(8):
        spread(e, "x").wait_send()
        spread(e, "y").wait_send()
        relay(e).wait_send()
        for q in range(4):
            to_sibling(e, q).wait_send()

    @pl.when(z < PLANES - 1)
    def _():
        each_chunk(lambda i, rows: hop_copy(i, rows).wait_send())

    @pl.when(z == PLANES - 1)
    def _():
        each_chunk(lambda i, rows: out_remote(i, rows).wait_send())
        each_chunk(lambda i, rows: out_local(i, rows).wait())

    @pl.when(z == 2)
    def _():
        each_chunk(lambda i, rows: out_remote(i, rows).wait_recv())


def solution(mesh):
    side_devs = mesh.shape["side"]
    tp_ways = side_devs // 2
    up_spec = P("side", None, "rep", None)
    down_spec = P("side", None, None, "rep")
    act_spec = P("side", "rep", None)

    def device_step(w_up, w_down, g_up, g_down, learn_rate, prompts, prompt_lens):
        new_up = w_up - learn_rate * g_up
        new_down = w_down - learn_rate * g_down
        upb = new_up[0].astype(jnp.bfloat16)
        dnb = new_down[0].astype(jnp.bfloat16)
        layers, width, ff = upb.shape
        tokens, d_half = prompts.shape[1:]
        model, hidden = width * REPS, ff * tp_ways
        chunk = min(256, tokens // 4)
        n_chunks = tokens // chunk + 2
        dma = pltpu.SemaphoreType.DMA
        hbm = pl.BlockSpec(memory_space=pltpu.HBM)
        y = pl.pallas_call(
            functools.partial(_pipeline_kernel, chunk=chunk, tile_n=min(512, ff), tile_m=min(512, d_half)),
            out_shape=jax.ShapeDtypeStruct((tokens, d_half), jnp.bfloat16),
            in_specs=[hbm, hbm, hbm],
            out_specs=hbm,
            scratch_shapes=[
                pltpu.VMEM((2, model, hidden), jnp.bfloat16),
                pltpu.VMEM((2, hidden, model), jnp.bfloat16),
                pltpu.VMEM((tokens, model), jnp.bfloat16),
                pltpu.VMEM((tokens, model), jnp.bfloat16),
                pltpu.VMEM((chunk, model), jnp.bfloat16),
                pltpu.VMEM((chunk, hidden), jnp.bfloat16),
                dma((8,)), dma((16,)), dma((8,)), dma((8,)), dma((8,)), dma((8,)),
                dma((8,)), dma((8,)), dma((32,)), dma((32,)),
                dma((2 * n_chunks,)), dma((n_chunks,)), dma((n_chunks,)), dma((n_chunks,)),
                dma((n_chunks,)), dma((n_chunks,)), dma((n_chunks,)),
            ],
            compiler_params=pltpu.CompilerParams(
                collective_id=0, has_side_effects=True, vmem_limit_bytes=60 * 1024 * 1024),
            name="layer_pipeline",
        )(upb, dnb, prompts[0])
        side_idx = lax.axis_index("side")
        keep = (jnp.arange(tokens)[:, None] < prompt_lens[0]) & (side_idx >= tp_ways)
        out_block = jnp.where(keep, y, jnp.zeros_like(y))
        return new_up, new_down, out_block[None]

    return jax.shard_map(
        device_step,
        mesh=mesh,
        in_specs=(up_spec, down_spec, up_spec, down_spec, P(), act_spec, P("rep")),
        out_specs=(up_spec, down_spec, act_spec),
        check_vma=False,
    )
```

```python
import functools

import jax
import jax.numpy as jnp
from jax import lax
from jax.experimental import pallas as pl
from jax.experimental.pallas import tpu as pltpu
from jax.sharding import PartitionSpec as P

MESH = pl.DeviceIdType.MESH
PLANES = 4
REPS = 8
UNITS = ((0, 0), (0, 1), (1, 0), (1, 1), (1, 2), (1, 3), (0, 2), (0, 3))


def _gelu(z):
    inner = 0.7978845608028654 * (z + 0.044715 * (z * z * z))
    return z * (0.5 * (1.0 + jnp.tanh(inner)))


def _pipeline_kernel(
    upb, dnb, x_ref, y_ref,
    wu, wd, hin, hout, mid, act,
    z_recv, z_send, x_recv, x_send, y_recv, y_send, d_recv, d_send, s_recv, s_send,
    in_recv, in_send, h_recv, h_send, out_recv, out_send, out_loc,
    *, chunk, tile_n, tile_m,
):
    z = lax.axis_index("side")
    r = lax.axis_index("rep")
    core = r % 2
    xpos = (r // 2) % 2
    ypos = r // 4
    r_x = r + 2 - 4 * xpos
    r_y = r + 4 - 8 * ypos
    r_d = r_x + 4 - 8 * ypos
    r_s = r + 1 - 2 * core

    width = upb.shape[1]
    ff = upb.shape[2]
    tokens, d_half = x_ref.shape
    first_rank = jnp.minimum(z, 1)
    n_chunks = tokens // chunk

    def dev(zz, rr):
        return (zz, rr)

    barrier = pltpu.get_barrier_semaphore()
    scope = jax.named_scope
    for step in range(1, PLANES):
        pl.semaphore_signal(barrier, inc=1, device_id=dev((z + step) % PLANES, r), device_id_type=MESH)
    for rr in (r_x, r_y, r_s):
        pl.semaphore_signal(barrier, inc=1, device_id=dev(z, rr), device_id_type=MESH)
    with scope("entry"):
        pl.semaphore_wait(barrier, PLANES + 2)

    def remote(src, dst, send, recv, to):
        return pltpu.make_async_remote_copy(
            src_ref=src, dst_ref=dst, send_sem=send, recv_sem=recv, device_id=to, device_id_type=MESH)

    def piece(jk, rank, rr):
        j, k = jk // 2, jk % 2
        off = pl.multiple_of(rr * width, width)
        if isinstance(rank, int):
            hid = pl.ds(rank * ff, ff)
        else:
            hid = pl.ds(pl.multiple_of(rank * ff, ff), ff)
        if k == 0:
            return wu.at[j, pl.ds(off, width), hid]
        return wd.at[j, hid, pl.ds(off, width)]

    def shard(jk, plane):
        src = upb if jk % 2 == 0 else dnb
        return src.at[2 * plane + jk // 2]

    def rows_of(i):
        return pl.ds(pl.multiple_of(i * chunk, chunk), chunk)

    def prompt_copy(i, rows):
        half = jnp.maximum(z - 2, 0)
        cols = pl.ds(pl.multiple_of(half * d_half, d_half), d_half)
        return remote(x_ref.at[rows, :], hin.at[rows, cols], in_send.at[i],
                      in_recv.at[half * n_chunks + i], dev(0, r))

    def each_chunk(fn):
        def body(i, carry):
            fn(i, rows_of(i))
            return carry
        lax.fori_loop(0, n_chunks, body, 0)

    def weight_copy(rank, plane, jk):
        e = UNITS.index((0 if rank == min(plane, 1) else 1, jk))
        if plane == rank:
            return pltpu.make_async_copy(shard(jk, plane), piece(jk, rank, r), z_recv.at[e])
        return remote(shard(jk, plane), piece(jk, rank, r), z_send.at[plane * 4 + jk],
                      z_recv.at[e], dev(plane, r))

    for rank in range(2):
        @pl.when(z == rank)
        def _():
            order = [(rank, jk) for jk in range(4)] + [(1 - rank, jk) for jk in range(4)]
            order += [(plane, jk) for jk in range(4) for plane in (2, 3)]
            for plane, jk in order:
                weight_copy(rank, plane, jk).start()

    def unit(e, rr):
        late, jk = UNITS[e]
        return piece(jk, 1 - first_rank if late else first_rank, rr)

    def spread(e, kind):
        own = unit(e, r)
        if kind == "x":
            return remote(own, own, x_send.at[e], x_recv.at[e], dev(z, r_x))
        return remote(own, own, y_send.at[e], y_recv.at[e], dev(z, r_y))

    def relay(e):
        if UNITS[e][1] % 2 == 0:
            ref, to = unit(e, r_x), r_y
        else:
            ref, to = unit(e, r_y), r_x
        return remote(ref, ref, d_send.at[e], d_recv.at[e], dev(z, to))

    def to_sibling(e, q):
        ref = unit(e, (r, r_x, r_y, r_d)[q])
        return remote(ref, ref, s_send.at[q * 8 + e], s_recv.at[q * 8 + e], dev(z, r_s))

    def landed(ref, sem):
        remote(ref, ref, sem, sem, dev(z, r_s)).wait_recv()

    def from_sibling(e, q):
        landed(unit(e, (r, r_x, r_y, r_d)[q] + 1 - 2 * core), s_recv.at[q * 8 + e])

    for i in range(8 + 4):
        if 0 <= i - 4:
            e = i - 4
            with scope(f"dw{e}"):
                landed(unit(e, r_d), d_recv.at[e])
            to_sibling(e, 3).start()
        if 0 <= i - 2 < 8:
            e = i - 2
            with scope(f"xw{e}"):
                landed(unit(e, r_x), x_recv.at[e])
                landed(unit(e, r_y), y_recv.at[e])
            relay(e).start()
            to_sibling(e, 1).start()
            to_sibling(e, 2).start()
        if i < 8:
            with scope(f"zw{i}"):
                landed(unit(i, r), z_recv.at[i])
            spread(i, "x").start()
            spread(i, "y").start()
            to_sibling(i, 0).start()
        if i == 2:
            @pl.when(z >= 2)
            def _():
                each_chunk(lambda c, rows: prompt_copy(c, rows).start())
    with scope("sib"):
        for e in range(8):
            for q in range(4):
                from_sibling(e, q)

    hidden = wu.shape[2]
    model = wu.shape[1]

    def hop_copy(i, rows):
        return remote(hout.at[rows, :], hin.at[rows, :], h_send.at[i], h_recv.at[i],
                      dev(jnp.minimum(z + 1, PLANES - 1), r))

    def out_remote(i, rows):
        return remote(hout.at[rows, pl.ds(0, d_half)], y_ref.at[rows, :], out_send.at[i], out_recv.at[i], dev(2, r))

    def out_local(i, rows):
        return pltpu.make_async_copy(hout.at[rows, pl.ds(d_half, d_half)], y_ref.at[rows, :], out_loc.at[i])

    def layer(j, src, src_rows, dst, dst_rows):
        for n in range(hidden // tile_n):
            cols = pl.ds(n * tile_n, tile_n)
            pre = jnp.dot(src[src_rows, :], wu[j, :, cols], preferred_element_type=jnp.float32)
            act[:, cols] = _gelu(pre).astype(jnp.bfloat16)
        for m in range(model // tile_m):
            cols = pl.ds(m * tile_m, tile_m)
            part = jnp.dot(act[...], wd[j, :, cols], preferred_element_type=jnp.float32)
            dst[dst_rows, cols] = (src[src_rows, cols].astype(jnp.float32) + part).astype(jnp.bfloat16)

    def chunk_step(i, carry):
        rows = rows_of(i)

        @pl.when(z == 0)
        def _():
            for half in range(2):
                landed(hin.at[rows, pl.ds(half * d_half, d_half)], in_recv.at[half * n_chunks + i])

        @pl.when(z > 0)
        def _():
            landed(hin.at[rows, :], h_recv.at[i])

        with scope("layers"):
            layer(0, hin, rows, mid, pl.ds(0, chunk))
            layer(1, mid, pl.ds(0, chunk), hout, rows)

        @pl.when(z < PLANES - 1)
        def _():
            hop_copy(i, rows).start()

        @pl.when(z == PLANES - 1)
        def _():
            out_remote(i, rows).start()
            out_local(i, rows).start()

        return carry

    lax.fori_loop(0, n_chunks, chunk_step, 0)

    @pl.when(z >= 2)
    def _():
        each_chunk(lambda i, rows: prompt_copy(i, rows).wait_send())

    for rank in range(2):
        @pl.when(z == rank)
        def _():
            for plane in range(PLANES):
                if plane != rank:
                    for jk in range(4):
                        weight_copy(rank, plane, jk).wait_send()

    for e in range(8):
        spread(e, "x").wait_send()
        spread(e, "y").wait_send()
        relay(e).wait_send()
        for q in range(4):
            to_sibling(e, q).wait_send()

    @pl.when(z < PLANES - 1)
    def _():
        each_chunk(lambda i, rows: hop_copy(i, rows).wait_send())

    @pl.when(z == PLANES - 1)
    def _():
        each_chunk(lambda i, rows: out_remote(i, rows).wait_send())
        each_chunk(lambda i, rows: out_local(i, rows).wait())

    @pl.when(z == 2)
    def _():
        each_chunk(lambda i, rows: out_remote(i, rows).wait_recv())


def solution(mesh):
    side_devs = mesh.shape["side"]
    tp_ways = side_devs // 2
    up_spec = P("side", None, "rep", None)
    down_spec = P("side", None, None, "rep")
    act_spec = P("side", "rep", None)

    def device_step(w_up, w_down, g_up, g_down, learn_rate, prompts, prompt_lens):
        new_up = w_up - learn_rate * g_up
        new_down = w_down - learn_rate * g_down
        upb = new_up[0].astype(jnp.bfloat16)
        dnb = new_down[0].astype(jnp.bfloat16)
        layers, width, ff = upb.shape
        tokens, d_half = prompts.shape[1:]
        model, hidden = width * REPS, ff * tp_ways
        chunk = min(128, tokens // 4)
        n_chunks = tokens // chunk
        dma = pltpu.SemaphoreType.DMA
        hbm = pl.BlockSpec(memory_space=pltpu.HBM)
        y = pl.pallas_call(
            functools.partial(_pipeline_kernel, chunk=chunk, tile_n=min(512, ff), tile_m=min(512, d_half)),
            out_shape=jax.ShapeDtypeStruct((tokens, d_half), jnp.bfloat16),
            in_specs=[hbm, hbm, hbm],
            out_specs=hbm,
            scratch_shapes=[
                pltpu.VMEM((2, model, hidden), jnp.bfloat16),
                pltpu.VMEM((2, hidden, model), jnp.bfloat16),
                pltpu.VMEM((tokens, model), jnp.bfloat16),
                pltpu.VMEM((tokens, model), jnp.bfloat16),
                pltpu.VMEM((chunk, model), jnp.bfloat16),
                pltpu.VMEM((chunk, hidden), jnp.bfloat16),
                dma((8,)), dma((16,)), dma((8,)), dma((8,)), dma((8,)), dma((8,)),
                dma((8,)), dma((8,)), dma((32,)), dma((32,)),
                dma((2 * n_chunks,)), dma((n_chunks,)), dma((n_chunks,)), dma((n_chunks,)),
                dma((n_chunks,)), dma((n_chunks,)), dma((n_chunks,)),
            ],
            compiler_params=pltpu.CompilerParams(
                collective_id=0, has_side_effects=True, vmem_limit_bytes=60 * 1024 * 1024),
            name="layer_pipeline",
        )(upb, dnb, prompts[0])
        side_idx = lax.axis_index("side")
        keep = (jnp.arange(tokens)[:, None] < prompt_lens[0]) & (side_idx >= tp_ways)
        out_block = jnp.where(keep, y, jnp.zeros_like(y))
        return new_up, new_down, out_block[None]

    return jax.shard_map(
        device_step,
        mesh=mesh,
        in_specs=(up_spec, down_spec, up_spec, down_spec, P(), act_spec, P("rep")),
        out_specs=(up_spec, down_spec, act_spec),
        check_vma=False,
    )
```

```python
import functools

import jax
import jax.numpy as jnp
from jax import lax
from jax.experimental import pallas as pl
from jax.experimental.pallas import tpu as pltpu
from jax.sharding import PartitionSpec as P

MESH = pl.DeviceIdType.MESH
PLANES = 4
REPS = 8
FIRST_RANK = (0, 1, 1, 0)
UNITS = tuple((late, jk) for late in range(2) for jk in range(4))


def _gelu(z):
    inner = 0.7978845608028654 * (z + 0.044715 * (z * z * z))
    return z * (0.5 * (1.0 + jnp.tanh(inner)))


def _pipeline_kernel(
    upb, dnb, x_ref, y_ref,
    wu, wd, hin, hout, mid, act,
    z_recv, z_send, x_recv, x_send, y_recv, y_send, d_recv, d_send, s_recv, s_send,
    in_recv, in_send, h_recv, h_send, out_recv, out_send, out_loc,
    *, chunk, tile_n, tile_m,
):
    z = lax.axis_index("side")
    r = lax.axis_index("rep")
    core = r % 2
    xpos = (r // 2) % 2
    ypos = r // 4
    r_x = r + 2 - 4 * xpos
    r_y = r + 4 - 8 * ypos
    r_d = r_x + 4 - 8 * ypos
    r_s = r + 1 - 2 * core

    width = upb.shape[1]
    ff = upb.shape[2]
    tokens, d_half = x_ref.shape
    first_rank = jnp.minimum(z, 1) - z // 3
    n_chunks = tokens // chunk

    def dev(zz, rr):
        return (zz, rr)

    barrier = pltpu.get_barrier_semaphore()
    scope = jax.named_scope
    for step in range(1, PLANES):
        pl.semaphore_signal(barrier, inc=1, device_id=dev((z + step) % PLANES, r), device_id_type=MESH)
    for rr in (r_x, r_y, r_s):
        pl.semaphore_signal(barrier, inc=1, device_id=dev(z, rr), device_id_type=MESH)
    with scope("entry"):
        pl.semaphore_wait(barrier, PLANES + 2)

    def remote(src, dst, send, recv, to):
        return pltpu.make_async_remote_copy(
            src_ref=src, dst_ref=dst, send_sem=send, recv_sem=recv, device_id=to, device_id_type=MESH)

    def piece(jk, rank, rr):
        j, k = jk // 2, jk % 2
        off = pl.multiple_of(rr * width, width)
        if isinstance(rank, int):
            hid = pl.ds(rank * ff, ff)
        else:
            hid = pl.ds(pl.multiple_of(rank * ff, ff), ff)
        if k == 0:
            return wu.at[j, pl.ds(off, width), hid]
        return wd.at[j, hid, pl.ds(off, width)]

    def shard(jk, plane):
        src = upb if jk % 2 == 0 else dnb
        return src.at[2 * plane + jk // 2]

    def rows_of(i):
        return pl.ds(pl.multiple_of(i * chunk, chunk), chunk)

    def prompt_copy(i, rows):
        half = jnp.maximum(z - 2, 0)
        cols = pl.ds(pl.multiple_of(half * d_half, d_half), d_half)
        return remote(x_ref.at[rows, :], hin.at[rows, cols], in_send.at[i],
                      in_recv.at[half * n_chunks + i], dev(0, r))

    def each_chunk(fn):
        def body(i, carry):
            fn(i, rows_of(i))
            return carry
        lax.fori_loop(0, n_chunks, body, 0)

    def weight_copy(rank, plane, jk):
        e = UNITS.index((0 if rank == FIRST_RANK[plane] else 1, jk))
        if plane == rank:
            return pltpu.make_async_copy(shard(jk, plane), piece(jk, rank, r), z_recv.at[e])
        return remote(shard(jk, plane), piece(jk, rank, r), z_send.at[plane * 4 + jk],
                      z_recv.at[e], dev(plane, r))

    for rank in range(2):
        @pl.when(z == rank)
        def _():
            order = [(rank, jk) for jk in range(4)] + [(1 - rank, jk) for jk in range(4)]
            if rank == 0:
                order += [(plane, jk) for jk in range(4) for plane in (3, 2)]
            else:
                order += [(plane, jk) for plane in (2, 3) for jk in range(4)]
            for plane, jk in order:
                weight_copy(rank, plane, jk).start()

    def unit(e, rr):
        late, jk = UNITS[e]
        return piece(jk, 1 - first_rank if late else first_rank, rr)

    def spread(e, kind):
        own = unit(e, r)
        if kind == "x":
            return remote(own, own, x_send.at[e], x_recv.at[e], dev(z, r_x))
        return remote(own, own, y_send.at[e], y_recv.at[e], dev(z, r_y))

    def relay(e):
        if UNITS[e][1] % 2 == 0:
            ref, to = unit(e, r_x), r_y
        else:
            ref, to = unit(e, r_y), r_x
        return remote(ref, ref, d_send.at[e], d_recv.at[e], dev(z, to))

    def to_sibling(e, q):
        ref = unit(e, (r, r_x, r_y, r_d)[q])
        return remote(ref, ref, s_send.at[q * 8 + e], s_recv.at[q * 8 + e], dev(z, r_s))

    def landed(ref, sem):
        remote(ref, ref, sem, sem, dev(z, r_s)).wait_recv()

    def from_sibling(e, q):
        landed(unit(e, (r, r_x, r_y, r_d)[q] + 1 - 2 * core), s_recv.at[q * 8 + e])

    for i in range(8 + 4):
        if 0 <= i - 4:
            e = i - 4
            with scope(f"dw{e}"):
                landed(unit(e, r_d), d_recv.at[e])
            to_sibling(e, 3).start()
        if 0 <= i - 2 < 8:
            e = i - 2
            with scope(f"xw{e}"):
                landed(unit(e, r_x), x_recv.at[e])
                landed(unit(e, r_y), y_recv.at[e])
            relay(e).start()
            to_sibling(e, 1).start()
            to_sibling(e, 2).start()
        if i < 8:
            with scope(f"zw{i}"):
                landed(unit(i, r), z_recv.at[i])
            spread(i, "x").start()
            spread(i, "y").start()
            to_sibling(i, 0).start()
        if i == 0 or i == 3:
            @pl.when(z == (3 if i == 0 else 2))
            def _():
                each_chunk(lambda c, rows: prompt_copy(c, rows).start())
    with scope("sib"):
        for e in range(8):
            for q in range(4):
                from_sibling(e, q)

    hidden = wu.shape[2]
    model = wu.shape[1]

    def hop_copy(i, rows):
        return remote(hout.at[rows, :], hin.at[rows, :], h_send.at[i], h_recv.at[i],
                      dev(jnp.minimum(z + 1, PLANES - 1), r))

    def out_remote(i, rows):
        return remote(hout.at[rows, pl.ds(0, d_half)], y_ref.at[rows, :], out_send.at[i], out_recv.at[i], dev(2, r))

    def out_local(i, rows):
        return pltpu.make_async_copy(hout.at[rows, pl.ds(d_half, d_half)], y_ref.at[rows, :], out_loc.at[i])

    def layer(j, src, src_rows, dst, dst_rows):
        for n in range(hidden // tile_n):
            cols = pl.ds(n * tile_n, tile_n)
            pre = jnp.dot(src[src_rows, :], wu[j, :, cols], preferred_element_type=jnp.float32)
            act[:, cols] = _gelu(pre).astype(jnp.bfloat16)
        for m in range(model // tile_m):
            cols = pl.ds(m * tile_m, tile_m)
            part = jnp.dot(act[...], wd[j, :, cols], preferred_element_type=jnp.float32)
            dst[dst_rows, cols] = (src[src_rows, cols].astype(jnp.float32) + part).astype(jnp.bfloat16)

    def drain_shards():
        @pl.when(z >= 2)
        def _():
            each_chunk(lambda i, rows: prompt_copy(i, rows).wait_send())

        for rank in range(2):
            @pl.when(z == rank)
            def _():
                for plane in range(PLANES):
                    if plane != rank:
                        for jk in range(4):
                            weight_copy(rank, plane, jk).wait_send()

        for e in range(8):
            spread(e, "x").wait_send()
            spread(e, "y").wait_send()
            relay(e).wait_send()
            for q in range(4):
                to_sibling(e, q).wait_send()

    def chunk_step(i, carry):
        rows = rows_of(i)

        @pl.when(i == n_chunks - 1)
        def _():
            drain_shards()

        @pl.when(z == 0)
        def _():
            for half in range(2):
                landed(hin.at[rows, pl.ds(half * d_half, d_half)], in_recv.at[half * n_chunks + i])

        @pl.when(z > 0)
        def _():
            landed(hin.at[rows, :], h_recv.at[i])

        with scope("layers"):
            layer(0, hin, rows, mid, pl.ds(0, chunk))
            layer(1, mid, pl.ds(0, chunk), hout, rows)

        @pl.when(z < PLANES - 1)
        def _():
            hop_copy(i, rows).start()

        @pl.when(z == PLANES - 1)
        def _():
            out_remote(i, rows).start()
            out_local(i, rows).start()

        return carry

    lax.fori_loop(0, n_chunks, chunk_step, 0)

    @pl.when(z < PLANES - 1)
    def _():
        each_chunk(lambda i, rows: hop_copy(i, rows).wait_send())

    @pl.when(z == PLANES - 1)
    def _():
        each_chunk(lambda i, rows: out_remote(i, rows).wait_send())
        each_chunk(lambda i, rows: out_local(i, rows).wait())

    @pl.when(z == 2)
    def _():
        each_chunk(lambda i, rows: out_remote(i, rows).wait_recv())


def solution(mesh):
    side_devs = mesh.shape["side"]
    tp_ways = side_devs // 2
    up_spec = P("side", None, "rep", None)
    down_spec = P("side", None, None, "rep")
    act_spec = P("side", "rep", None)

    def device_step(w_up, w_down, g_up, g_down, learn_rate, prompts, prompt_lens):
        new_up = w_up - learn_rate * g_up
        new_down = w_down - learn_rate * g_down
        upb = new_up[0].astype(jnp.bfloat16)
        dnb = new_down[0].astype(jnp.bfloat16)
        layers, width, ff = upb.shape
        tokens, d_half = prompts.shape[1:]
        model, hidden = width * REPS, ff * tp_ways
        chunk = min(128, tokens // 4)
        n_chunks = tokens // chunk
        dma = pltpu.SemaphoreType.DMA
        hbm = pl.BlockSpec(memory_space=pltpu.HBM)
        y = pl.pallas_call(
            functools.partial(_pipeline_kernel, chunk=chunk, tile_n=min(512, ff), tile_m=min(512, d_half)),
            out_shape=jax.ShapeDtypeStruct((tokens, d_half), jnp.bfloat16),
            in_specs=[hbm, hbm, hbm],
            out_specs=hbm,
            scratch_shapes=[
                pltpu.VMEM((2, model, hidden), jnp.bfloat16),
                pltpu.VMEM((2, hidden, model), jnp.bfloat16),
                pltpu.VMEM((tokens, model), jnp.bfloat16),
                pltpu.VMEM((tokens, model), jnp.bfloat16),
                pltpu.VMEM((chunk, model), jnp.bfloat16),
                pltpu.VMEM((chunk, hidden), jnp.bfloat16),
                dma((8,)), dma((16,)), dma((8,)), dma((8,)), dma((8,)), dma((8,)),
                dma((8,)), dma((8,)), dma((32,)), dma((32,)),
                dma((2 * n_chunks,)), dma((n_chunks,)), dma((n_chunks,)), dma((n_chunks,)),
                dma((n_chunks,)), dma((n_chunks,)), dma((n_chunks,)),
            ],
            compiler_params=pltpu.CompilerParams(
                collective_id=0, has_side_effects=True, vmem_limit_bytes=60 * 1024 * 1024),
            name="layer_pipeline",
        )(upb, dnb, prompts[0])
        side_idx = lax.axis_index("side")
        keep = (jnp.arange(tokens)[:, None] < prompt_lens[0]) & (side_idx >= tp_ways)
        out_block = jnp.where(keep, y, jnp.zeros_like(y))
        return new_up, new_down, out_block[None]

    return jax.shard_map(
        device_step,
        mesh=mesh,
        in_specs=(up_spec, down_spec, up_spec, down_spec, P(), act_spec, P("rep")),
        out_specs=(up_spec, down_spec, act_spec),
        check_vma=False,
    )
```

```python
import functools

import jax
import jax.numpy as jnp
from jax import lax
from jax.experimental import pallas as pl
from jax.experimental.pallas import tpu as pltpu
from jax.sharding import PartitionSpec as P

MESH = pl.DeviceIdType.MESH
PLANES = 4
REPS = 8
FIRST_RANK = (0, 1, 1, 0)
UNITS = tuple((late, jk) for late in range(2) for jk in range(4))
SEND_ORDER = tuple(
    tuple((plane, jk + n) for plane, jk in pairs for n in range(2))
    for pairs in (
        ((0, 0), (1, 0), (0, 2), (1, 2), (3, 0), (2, 0), (3, 2), (2, 2)),
        ((2, 0), (1, 0), (0, 0), (2, 2), (1, 2), (0, 2), (3, 0), (3, 2)),
    )
)


def _gelu(z):
    inner = 0.7978845608028654 * (z + 0.044715 * (z * z * z))
    return z * (0.5 * (1.0 + jnp.tanh(inner)))


def _pipeline_kernel(
    lr, w_up, w_down, g_up, g_down, x_ref, _, y_ref,
    wu, wd, hin, hout, mid, act, up_out, down_out, up_in, down_in, fetch_sem,
    z_recv, z_send, x_recv, x_send, y_recv, y_send, d_recv, d_send, s_recv, s_send,
    in_recv, in_send, h_recv, h_send, out_recv, out_send, out_loc,
    *, chunk, tile_n, tile_m,
):
    z = lax.axis_index("side")
    r = lax.axis_index("rep")
    core = r % 2
    xpos = (r // 2) % 2
    ypos = r // 4
    r_x = r + 2 - 4 * xpos
    r_y = r + 4 - 8 * ypos
    r_d = r_x + 4 - 8 * ypos
    r_s = r + 1 - 2 * core

    width, ff = w_up.shape[1:]
    tokens, d_half = x_ref.shape
    first_rank = jnp.minimum(z, 1) - z // 3
    n_chunks = tokens // chunk

    def dev(zz, rr):
        return (zz, rr)

    barrier = pltpu.get_barrier_semaphore()
    scope = jax.named_scope
    for step in range(1, PLANES):
        pl.semaphore_signal(barrier, inc=1, device_id=dev((z + step) % PLANES, r), device_id_type=MESH)
    for rr in (r_x, r_y, r_s):
        pl.semaphore_signal(barrier, inc=1, device_id=dev(z, rr), device_id_type=MESH)
    def remote(src, dst, send, recv, to):
        return pltpu.make_async_remote_copy(
            src_ref=src, dst_ref=dst, send_sem=send, recv_sem=recv, device_id=to, device_id_type=MESH)

    def piece(jk, rank, rr):
        j, k = jk // 2, jk % 2
        off = pl.multiple_of(rr * width, width)
        if isinstance(rank, int):
            hid = pl.ds(rank * ff, ff)
        else:
            hid = pl.ds(pl.multiple_of(rank * ff, ff), ff)
        if k == 0:
            return wu.at[j, pl.ds(off, width), hid]
        return wd.at[j, hid, pl.ds(off, width)]

    def shard(jk, plane):
        src = up_out if jk % 2 == 0 else down_out
        return src.at[2 * plane + jk // 2]

    def rows_of(i):
        return pl.ds(pl.multiple_of(i * chunk, chunk), chunk)

    def prompt_copy(i, rows):
        half = jnp.maximum(z - 2, 0)
        cols = pl.ds(pl.multiple_of(half * d_half, d_half), d_half)
        return remote(x_ref.at[rows, :], hin.at[rows, cols], in_send.at[i],
                      in_recv.at[half * n_chunks + i], dev(0, r))

    def each_chunk(fn):
        def body(i, carry):
            fn(i, rows_of(i))
            return carry
        lax.fori_loop(0, n_chunks, body, 0)

    def unit(e, rr):
        late, jk = UNITS[e]
        return piece(jk, 1 - first_rank if late else first_rank, rr)

    def spread(e, kind):
        own = unit(e, r)
        if kind == "x":
            return remote(own, own, x_send.at[e], x_recv.at[e], dev(z, r_x))
        return remote(own, own, y_send.at[e], y_recv.at[e], dev(z, r_y))

    def relay(e):
        if UNITS[e][1] % 2 == 0:
            ref, to = unit(e, r_x), r_y
        else:
            ref, to = unit(e, r_y), r_x
        return remote(ref, ref, d_send.at[e], d_recv.at[e], dev(z, to))

    def to_sibling(e, q):
        ref = unit(e, (r, r_x, r_y, r_d)[q])
        return remote(ref, ref, s_send.at[q * 8 + e], s_recv.at[q * 8 + e], dev(z, r_s))

    def landed(ref, sem):
        remote(ref, ref, sem, sem, dev(z, r_s)).wait_recv()

    def from_sibling(e, q):
        landed(unit(e, (r, r_x, r_y, r_d)[q] + 1 - 2 * core), s_recv.at[q * 8 + e])

    def weight_copy(rank, plane, jk):
        e = UNITS.index((0 if rank == FIRST_RANK[plane] else 1, jk))
        return remote(shard(jk, plane), piece(jk, rank, r), z_send.at[plane * 4 + jk],
                      z_recv.at[e], dev(plane, r))

    def fetches(rank, q):
        plane, jk = SEND_ORDER[rank][q]
        layer_idx, slot = 2 * plane + jk // 2, q // 2 % 2
        srcs, dst = ((w_up, g_up), up_in) if jk % 2 == 0 else ((w_down, g_down), down_in)
        return [pltpu.make_async_copy(srcs[n].at[layer_idx], dst.at[slot, n], fetch_sem.at[jk % 2, slot, n])
                for n in range(2)]

    def fetch(rank, q):
        for copy in fetches(rank, q):
            copy.start()

    def update(rank, q):
        plane, jk = SEND_ORDER[rank][q]
        slot = q // 2 % 2
        for copy in fetches(rank, q):
            copy.wait()
        src, total = (up_in, width) if jk % 2 == 0 else (down_in, ff)
        block = 16 if jk % 2 == 0 else min(128, ff)

        def body(b, carry):
            rows = pl.ds(pl.multiple_of(b * block, block), block)
            new = (src[slot, 0, rows, :] - lr[0] * src[slot, 1, rows, :]).astype(jnp.bfloat16)
            if plane != rank:
                shard(jk, plane)[rows, :] = new
            elif jk % 2 == 0:
                off = pl.multiple_of(r * width + b * block, block)
                wu[jk // 2, pl.ds(off, block), pl.ds(rank * ff, ff)] = new
            else:
                off = pl.multiple_of(rank * ff + b * block, block)
                wd[jk // 2, pl.ds(off, block), pl.ds(pl.multiple_of(r * width, width), width)] = new
            return carry
        lax.fori_loop(0, total // block, body, 0)

    def issue(rank, q):
        plane, jk = SEND_ORDER[rank][q]
        if plane != rank:
            weight_copy(rank, plane, jk).start()
        else:
            spread(jk, "x").start()
            spread(jk, "y").start()
            to_sibling(jk, 0).start()

    n_units = len(SEND_ORDER[0])
    for rank in range(2):
        @pl.when(z == rank)
        def _():
            for q in range(4):
                fetch(rank, q)
            for q in range(2):
                update(rank, q)
                fetch(rank, q + 4)

    with scope("entry"):
        pl.semaphore_wait(barrier, PLANES + 2)

    for rank in range(2):
        @pl.when(z == rank)
        def _():
            issue(rank, 0)
            for q in range(2, n_units):
                update(rank, q)
                if q + 4 < n_units:
                    fetch(rank, q + 4)
                issue(rank, q - 1)
            issue(rank, n_units - 1)

    for i in range(8 + 4):
        if 0 <= i - 4:
            e = i - 4
            with scope(f"dw{e}"):
                landed(unit(e, r_d), d_recv.at[e])
            to_sibling(e, 3).start()
        if 0 <= i - 2 < 8:
            e = i - 2
            with scope(f"xw{e}"):
                landed(unit(e, r_x), x_recv.at[e])
                landed(unit(e, r_y), y_recv.at[e])
            relay(e).start()
            to_sibling(e, 1).start()
            to_sibling(e, 2).start()
        if i < 8:
            def pass_on(e):
                with scope(f"zw{e}"):
                    landed(unit(e, r), z_recv.at[e])
                spread(e, "x").start()
                spread(e, "y").start()
                to_sibling(e, 0).start()

            if i < 4:
                pl.when(z >= 2)(functools.partial(pass_on, i))
            else:
                pass_on(i)
        if i == 0 or i == 3:
            @pl.when(z == (3 if i == 0 else 2))
            def _():
                each_chunk(lambda c, rows: prompt_copy(c, rows).start())
    with scope("sib"):
        for e in range(8):
            for q in range(4):
                from_sibling(e, q)

    hidden = wu.shape[2]
    model = wu.shape[1]

    def hop_copy(i, rows):
        return remote(hout.at[rows, :], hin.at[rows, :], h_send.at[i], h_recv.at[i],
                      dev(jnp.minimum(z + 1, PLANES - 1), r))

    def out_remote(i, rows):
        return remote(hout.at[rows, pl.ds(0, d_half)], y_ref.at[rows, :], out_send.at[i], out_recv.at[i], dev(2, r))

    def out_local(i, rows):
        return pltpu.make_async_copy(hout.at[rows, pl.ds(d_half, d_half)], y_ref.at[rows, :], out_loc.at[i])

    def layer(j, src, src_rows, dst, dst_rows):
        for n in range(hidden // tile_n):
            cols = pl.ds(n * tile_n, tile_n)
            pre = jnp.dot(src[src_rows, :], wu[j, :, cols], preferred_element_type=jnp.float32)
            act[:, cols] = _gelu(pre).astype(jnp.bfloat16)
        for m in range(model // tile_m):
            cols = pl.ds(m * tile_m, tile_m)
            part = jnp.dot(act[...], wd[j, :, cols], preferred_element_type=jnp.float32)
            dst[dst_rows, cols] = (src[src_rows, cols].astype(jnp.float32) + part).astype(jnp.bfloat16)

    def drain_shards():
        @pl.when(z >= 2)
        def _():
            each_chunk(lambda i, rows: prompt_copy(i, rows).wait_send())

        for rank in range(2):
            @pl.when(z == rank)
            def _():
                for plane in range(PLANES):
                    if plane != rank:
                        for jk in range(4):
                            weight_copy(rank, plane, jk).wait_send()

        for e in range(8):
            spread(e, "x").wait_send()
            spread(e, "y").wait_send()
            relay(e).wait_send()
            for q in range(4):
                to_sibling(e, q).wait_send()

    def chunk_step(i, carry):
        rows = rows_of(i)

        @pl.when(i == n_chunks - 1)
        def _():
            drain_shards()

        @pl.when(z == 0)
        def _():
            for half in range(2):
                landed(hin.at[rows, pl.ds(half * d_half, d_half)], in_recv.at[half * n_chunks + i])

        @pl.when(z > 0)
        def _():
            landed(hin.at[rows, :], h_recv.at[i])

        with scope("layers"):
            layer(0, hin, rows, mid, pl.ds(0, chunk))
            layer(1, mid, pl.ds(0, chunk), hout, rows)

        @pl.when(z < PLANES - 1)
        def _():
            hop_copy(i, rows).start()

        @pl.when(z == PLANES - 1)
        def _():
            out_remote(i, rows).start()
            out_local(i, rows).start()

        return carry

    lax.fori_loop(0, n_chunks, chunk_step, 0)

    @pl.when(z < PLANES - 1)
    def _():
        each_chunk(lambda i, rows: hop_copy(i, rows).wait_send())

    @pl.when(z == PLANES - 1)
    def _():
        each_chunk(lambda i, rows: out_remote(i, rows).wait_send())
        each_chunk(lambda i, rows: out_local(i, rows).wait())

    @pl.when(z == 2)
    def _():
        each_chunk(lambda i, rows: out_remote(i, rows).wait_recv())


def _zeros_kernel(up_ref, down_ref, tok_ref, up_zero, down_zero, sem):
    tok_ref[...] = jnp.zeros_like(tok_ref)

    @pl.when(lax.axis_index("side") >= PLANES // 2)
    def _():
        up_zero[...] = jnp.zeros_like(up_zero)
        down_zero[...] = jnp.zeros_like(down_zero)
        copies = []
        for n in range(up_ref.shape[0]):
            copies.append(pltpu.make_async_copy(up_zero, up_ref.at[n], sem.at[0, n]))
            copies.append(pltpu.make_async_copy(down_zero, down_ref.at[n], sem.at[1, n]))
        for copy in copies:
            copy.start()
        for copy in copies:
            copy.wait()


def _finish_kernel(
    lr, lens, w_up, w_down, g_up, g_down, y_ref, _up, _down,
    up_ref, down_ref, out_ref,
    up_in, down_in, up_out, down_out, y_buf, in_sem, out_sem, y_in_sem, y_out_sem,
):
    z = lax.axis_index("side")
    tokens = y_ref.shape[0]
    n_parts = y_in_sem.shape[0]
    part = tokens // n_parts

    def y_copy(n, out):
        rows = pl.ds(n * part, part)
        if out:
            return pltpu.make_async_copy(y_buf.at[rows, :], out_ref.at[rows, :], y_out_sem.at[n])
        return pltpu.make_async_copy(y_ref.at[rows, :], y_buf.at[rows, :], y_in_sem.at[n])

    @pl.when(z >= PLANES // 2)
    def _():
        for n in range(n_parts):
            y_copy(n, False).start()
        for n in range(n_parts):
            y_copy(n, False).wait()
            rows = pl.ds(n * part, part)
            row_idx = n * part + lax.broadcasted_iota(jnp.int32, (part, 1), 0)
            y_buf[rows, :] = jnp.where(row_idx < lens[0], y_buf[rows, :], jnp.zeros((), y_buf.dtype))
            y_copy(n, True).start()
        for n in range(n_parts):
            y_copy(n, True).wait()

    @pl.when(z < PLANES // 2)
    def _():
        y_buf[...] = jnp.zeros_like(y_buf)
        for n in range(n_parts):
            y_copy(n, True).start()
        layers = w_up.shape[0]
        kinds = ((w_up, g_up, up_in, up_out, up_ref, 16), (w_down, g_down, down_in, down_out, down_ref, 128))

        def loads(n, k, slot):
            w, g, buf = kinds[k][:3]
            return [pltpu.make_async_copy(src.at[n], buf.at[slot, m], in_sem.at[k, slot, m])
                    for m, src in enumerate((w, g))]

        def store(n, k, slot):
            return pltpu.make_async_copy(kinds[k][3].at[slot], kinds[k][4].at[n], out_sem.at[k, slot])

        for k in range(2):
            for n in range(2):
                for copy in loads(n, k, n):
                    copy.start()

        def body(n, carry):
            slot = n % 2
            for k in range(2):
                for copy in loads(n, k, slot):
                    copy.wait()

                @pl.when(n >= 2)
                def _():
                    store(n - 2, k, slot).wait()

                src, dst, block = kinds[k][2], kinds[k][3], kinds[k][5]
                block = min(block, src.shape[2])

                def rows_body(b, c):
                    rows = pl.ds(pl.multiple_of(b * block, block), block)
                    dst[slot, rows, :] = src[slot, 0, rows, :] - lr[0] * src[slot, 1, rows, :]
                    return c
                lax.fori_loop(0, src.shape[2] // block, rows_body, 0)
                store(n, k, slot).start()

                @pl.when(n + 2 < layers)
                def _():
                    for copy in loads(n + 2, k, slot):
                        copy.start()
            return carry
        lax.fori_loop(0, layers, body, 0)
        for n in (layers - 2, layers - 1):
            for k in range(2):
                store(n, k, n % 2).wait()
        for n in range(n_parts):
            y_copy(n, True).wait()


def solution(mesh):
    tp_ways = mesh.shape["side"] // 2
    up_spec = P("side", None, "rep", None)
    down_spec = P("side", None, None, "rep")
    act_spec = P("side", "rep", None)

    def device_step(w_up, w_down, g_up, g_down, learn_rate, prompts, prompt_lens):
        w_up, w_down, g_up, g_down = w_up[0], w_down[0], g_up[0], g_down[0]
        layers, width, ff = w_up.shape
        tokens, d_half = prompts.shape[1:]
        model, hidden = width * REPS, ff * tp_ways
        chunk = min(128, tokens // 4)
        n_chunks = tokens // chunk
        dma = pltpu.SemaphoreType.DMA
        hbm = pl.BlockSpec(memory_space=pltpu.HBM)
        smem = pl.BlockSpec(memory_space=pltpu.SMEM)
        lr = learn_rate.reshape(1)
        up_shape = jax.ShapeDtypeStruct(w_up.shape, jnp.float32)
        down_shape = jax.ShapeDtypeStruct(w_down.shape, jnp.float32)
        y_shape = jax.ShapeDtypeStruct((tokens, d_half), jnp.bfloat16)
        up_in = pltpu.VMEM((2, 2, width, ff), jnp.float32)
        down_in = pltpu.VMEM((2, 2, ff, width), jnp.float32)

        new_up, new_down, token = pl.pallas_call(
            _zeros_kernel,
            out_shape=(up_shape, down_shape, jax.ShapeDtypeStruct((8, 128), jnp.float32)),
            out_specs=(hbm, hbm, pl.BlockSpec(memory_space=pltpu.VMEM)),
            scratch_shapes=[
                pltpu.VMEM((width, ff), jnp.float32), pltpu.VMEM((ff, width), jnp.float32), dma((2, layers))],
            compiler_params=pltpu.CompilerParams(vmem_limit_bytes=16 * 1024 * 1024),
            name="zeros",
        )()
        y = pl.pallas_call(
            functools.partial(_pipeline_kernel, chunk=chunk, tile_n=min(512, ff), tile_m=min(512, d_half)),
            out_shape=y_shape,
            in_specs=[smem] + [hbm] * 6,
            out_specs=hbm,
            scratch_shapes=[
                pltpu.VMEM((2, model, hidden), jnp.bfloat16),
                pltpu.VMEM((2, hidden, model), jnp.bfloat16),
                pltpu.VMEM((tokens, model), jnp.bfloat16),
                pltpu.VMEM((tokens, model), jnp.bfloat16),
                pltpu.VMEM((chunk, model), jnp.bfloat16),
                pltpu.VMEM((chunk, hidden), jnp.bfloat16),
                pltpu.VMEM((layers, width, ff), jnp.bfloat16),
                pltpu.VMEM((layers, ff, width), jnp.bfloat16),
                up_in, down_in, dma((2, 2, 2)),
                dma((8,)), dma((16,)), dma((8,)), dma((8,)), dma((8,)), dma((8,)),
                dma((8,)), dma((8,)), dma((32,)), dma((32,)),
                dma((2 * n_chunks,)), dma((n_chunks,)), dma((n_chunks,)), dma((n_chunks,)),
                dma((n_chunks,)), dma((n_chunks,)), dma((n_chunks,)),
            ],
            compiler_params=pltpu.CompilerParams(
                collective_id=0, has_side_effects=True, vmem_limit_bytes=62 * 1024 * 1024),
            name="layer_pipeline",
        )(lr, w_up, w_down, g_up, g_down, prompts[0], token)
        new_up, new_down, out = pl.pallas_call(
            _finish_kernel,
            out_shape=(up_shape, down_shape, y_shape),
            in_specs=[smem] * 2 + [hbm] * 7,
            out_specs=(hbm, hbm, hbm),
            scratch_shapes=[
                up_in, down_in,
                pltpu.VMEM((2, width, ff), jnp.float32), pltpu.VMEM((2, ff, width), jnp.float32),
                pltpu.VMEM((tokens, d_half), jnp.bfloat16),
                dma((2, 2, 2)), dma((2, 2)), dma((4,)), dma((4,)),
            ],
            input_output_aliases={7: 0, 8: 1},
            compiler_params=pltpu.CompilerParams(vmem_limit_bytes=32 * 1024 * 1024),
            name="finish",
        )(lr, prompt_lens, w_up, w_down, g_up, g_down, y, new_up, new_down)
        return new_up[None], new_down[None], out[None]

    return jax.shard_map(
        device_step,
        mesh=mesh,
        in_specs=(up_spec, down_spec, up_spec, down_spec, P(), act_spec, P("rep")),
        out_specs=(up_spec, down_spec, act_spec),
        check_vma=False,
    )
```

```python
import functools

import jax
import jax.numpy as jnp
from jax import lax
from jax.experimental import pallas as pl
from jax.experimental.pallas import tpu as pltpu
from jax.sharding import PartitionSpec as P

MESH = pl.DeviceIdType.MESH
PLANES = 4
REPS = 8
FIRST_RANK = (0, 1, 1, 0)
UNITS = tuple((late, jk) for late in range(2) for jk in range(4))
SEND_ORDER = tuple(
    tuple((plane, jk + n) for plane, jk in pairs for n in range(2))
    for pairs in (
        ((0, 0), (1, 0), (0, 2), (1, 2), (3, 0), (2, 0), (3, 2), (2, 2)),
        ((2, 0), (1, 0), (0, 0), (2, 2), (1, 2), (0, 2), (3, 0), (3, 2)),
    )
)


def _gelu(z):
    inner = 0.7978845608028654 * (z + 0.044715 * (z * z * z))
    return z * (0.5 * (1.0 + jnp.tanh(inner)))


def _pipeline_kernel(
    lr, w_up, w_down, g_up, g_down, x_ref, y_ref,
    wu, wd, hin, hout, mid, act, up_out, down_out, up_in, down_in, fetch_sem,
    z_recv, z_send, x_recv, x_send, y_recv, y_send, d_recv, d_send, s_recv, s_send,
    in_recv, in_send, h_recv, h_send, out_recv, out_send, out_loc,
    *, chunk, tile_n, tile_m,
):
    z = lax.axis_index("side")
    r = lax.axis_index("rep")
    core = r % 2
    xpos = (r // 2) % 2
    ypos = r // 4
    r_x = r + 2 - 4 * xpos
    r_y = r + 4 - 8 * ypos
    r_d = r_x + 4 - 8 * ypos
    r_s = r + 1 - 2 * core

    width, ff = w_up.shape[1:]
    tokens, d_half = x_ref.shape
    first_rank = jnp.minimum(z, 1) - z // 3
    n_chunks = tokens // chunk

    def dev(zz, rr):
        return (zz, rr)

    barrier = pltpu.get_barrier_semaphore()
    scope = jax.named_scope
    for step in range(1, PLANES):
        pl.semaphore_signal(barrier, inc=1, device_id=dev((z + step) % PLANES, r), device_id_type=MESH)
    for rr in (r_x, r_y, r_s):
        pl.semaphore_signal(barrier, inc=1, device_id=dev(z, rr), device_id_type=MESH)
    def remote(src, dst, send, recv, to):
        return pltpu.make_async_remote_copy(
            src_ref=src, dst_ref=dst, send_sem=send, recv_sem=recv, device_id=to, device_id_type=MESH)

    def piece(jk, rank, rr):
        j, k = jk // 2, jk % 2
        off = pl.multiple_of(rr * width, width)
        if isinstance(rank, int):
            hid = pl.ds(rank * ff, ff)
        else:
            hid = pl.ds(pl.multiple_of(rank * ff, ff), ff)
        if k == 0:
            return wu.at[j, pl.ds(off, width), hid]
        return wd.at[j, hid, pl.ds(off, width)]

    def shard(jk, plane):
        src = up_out if jk % 2 == 0 else down_out
        return src.at[2 * plane + jk // 2]

    def rows_of(i):
        return pl.ds(pl.multiple_of(i * chunk, chunk), chunk)

    def prompt_copy(i, rows):
        half = jnp.maximum(z - 2, 0)
        cols = pl.ds(pl.multiple_of(half * d_half, d_half), d_half)
        return remote(x_ref.at[rows, :], hin.at[rows, cols], in_send.at[i],
                      in_recv.at[half * n_chunks + i], dev(0, r))

    def each_chunk(fn):
        def body(i, carry):
            fn(i, rows_of(i))
            return carry
        lax.fori_loop(0, n_chunks, body, 0)

    def unit(e, rr):
        late, jk = UNITS[e]
        return piece(jk, 1 - first_rank if late else first_rank, rr)

    def spread(e, kind):
        own = unit(e, r)
        if kind == "x":
            return remote(own, own, x_send.at[e], x_recv.at[e], dev(z, r_x))
        return remote(own, own, y_send.at[e], y_recv.at[e], dev(z, r_y))

    def relay(e):
        if UNITS[e][1] % 2 == 0:
            ref, to = unit(e, r_x), r_y
        else:
            ref, to = unit(e, r_y), r_x
        return remote(ref, ref, d_send.at[e], d_recv.at[e], dev(z, to))

    def to_sibling(e, q):
        ref = unit(e, (r, r_x, r_y, r_d)[q])
        return remote(ref, ref, s_send.at[q * 8 + e], s_recv.at[q * 8 + e], dev(z, r_s))

    def landed(ref, sem):
        remote(ref, ref, sem, sem, dev(z, r_s)).wait_recv()

    def from_sibling(e, q):
        landed(unit(e, (r, r_x, r_y, r_d)[q] + 1 - 2 * core), s_recv.at[q * 8 + e])

    def weight_copy(rank, plane, jk):
        e = UNITS.index((0 if rank == FIRST_RANK[plane] else 1, jk))
        return remote(shard(jk, plane), piece(jk, rank, r), z_send.at[plane * 4 + jk],
                      z_recv.at[e], dev(plane, r))

    def fetches(rank, q):
        plane, jk = SEND_ORDER[rank][q]
        layer_idx, slot = 2 * plane + jk // 2, q // 2 % 2
        srcs, dst = ((w_up, g_up), up_in) if jk % 2 == 0 else ((w_down, g_down), down_in)
        return [pltpu.make_async_copy(srcs[n].at[layer_idx], dst.at[slot, n], fetch_sem.at[jk % 2, slot, n])
                for n in range(2)]

    def fetch(rank, q):
        for copy in fetches(rank, q):
            copy.start()

    def update(rank, q):
        plane, jk = SEND_ORDER[rank][q]
        slot = q // 2 % 2
        for copy in fetches(rank, q):
            copy.wait()
        src, total = (up_in, width) if jk % 2 == 0 else (down_in, ff)
        block = 16 if jk % 2 == 0 else min(128, ff)

        def body(b, carry):
            rows = pl.ds(pl.multiple_of(b * block, block), block)
            new = (src[slot, 0, rows, :] - lr[0] * src[slot, 1, rows, :]).astype(jnp.bfloat16)
            if plane != rank:
                shard(jk, plane)[rows, :] = new
            elif jk % 2 == 0:
                off = pl.multiple_of(r * width + b * block, block)
                wu[jk // 2, pl.ds(off, block), pl.ds(rank * ff, ff)] = new
            else:
                off = pl.multiple_of(rank * ff + b * block, block)
                wd[jk // 2, pl.ds(off, block), pl.ds(pl.multiple_of(r * width, width), width)] = new
            return carry
        lax.fori_loop(0, total // block, body, 0)

    def issue(rank, q):
        plane, jk = SEND_ORDER[rank][q]
        if plane != rank:
            weight_copy(rank, plane, jk).start()
        else:
            spread(jk, "x").start()
            spread(jk, "y").start()
            to_sibling(jk, 0).start()

    n_units = len(SEND_ORDER[0])
    for rank in range(2):
        @pl.when(z == rank)
        def _():
            for q in range(4):
                fetch(rank, q)
            for q in range(2):
                update(rank, q)
                fetch(rank, q + 4)

    with scope("entry"):
        pl.semaphore_wait(barrier, PLANES + 2)

    for rank in range(2):
        @pl.when(z == rank)
        def _():
            issue(rank, 0)
            for q in range(2, n_units):
                update(rank, q)
                if q + 4 < n_units:
                    fetch(rank, q + 4)
                issue(rank, q - 1)
            issue(rank, n_units - 1)

    for i in range(8 + 4):
        if 0 <= i - 4:
            e = i - 4
            with scope(f"dw{e}"):
                landed(unit(e, r_d), d_recv.at[e])
            to_sibling(e, 3).start()
        if 0 <= i - 2 < 8:
            e = i - 2
            with scope(f"xw{e}"):
                landed(unit(e, r_x), x_recv.at[e])
                landed(unit(e, r_y), y_recv.at[e])
            relay(e).start()
            to_sibling(e, 1).start()
            to_sibling(e, 2).start()
        if i < 8:
            def pass_on(e):
                with scope(f"zw{e}"):
                    landed(unit(e, r), z_recv.at[e])
                spread(e, "x").start()
                spread(e, "y").start()
                to_sibling(e, 0).start()

            if i < 4:
                pl.when(z >= 2)(functools.partial(pass_on, i))
            else:
                pass_on(i)
        if i == 0 or i == 3:
            @pl.when(z == (3 if i == 0 else 2))
            def _():
                each_chunk(lambda c, rows: prompt_copy(c, rows).start())
    with scope("sib"):
        for e in range(8):
            for q in range(4):
                from_sibling(e, q)

    hidden = wu.shape[2]
    model = wu.shape[1]

    def hop_copy(i, rows):
        return remote(hout.at[rows, :], hin.at[rows, :], h_send.at[i], h_recv.at[i],
                      dev(jnp.minimum(z + 1, PLANES - 1), r))

    def out_remote(i, rows):
        return remote(hout.at[rows, pl.ds(0, d_half)], y_ref.at[rows, :], out_send.at[i], out_recv.at[i], dev(2, r))

    def out_local(i, rows):
        return pltpu.make_async_copy(hout.at[rows, pl.ds(d_half, d_half)], y_ref.at[rows, :], out_loc.at[i])

    def layer(j, src, src_rows, dst, dst_rows):
        for n in range(hidden // tile_n):
            cols = pl.ds(n * tile_n, tile_n)
            pre = jnp.dot(src[src_rows, :], wu[j, :, cols], preferred_element_type=jnp.float32)
            act[:, cols] = _gelu(pre).astype(jnp.bfloat16)
        for m in range(model // tile_m):
            cols = pl.ds(m * tile_m, tile_m)
            part = jnp.dot(act[...], wd[j, :, cols], preferred_element_type=jnp.float32)
            dst[dst_rows, cols] = (src[src_rows, cols].astype(jnp.float32) + part).astype(jnp.bfloat16)

    def drain_shards():
        @pl.when(z >= 2)
        def _():
            each_chunk(lambda i, rows: prompt_copy(i, rows).wait_send())

        for rank in range(2):
            @pl.when(z == rank)
            def _():
                for plane in range(PLANES):
                    if plane != rank:
                        for jk in range(4):
                            weight_copy(rank, plane, jk).wait_send()

        for e in range(8):
            spread(e, "x").wait_send()
            spread(e, "y").wait_send()
            relay(e).wait_send()
            for q in range(4):
                to_sibling(e, q).wait_send()

    def chunk_step(i, carry):
        rows = rows_of(i)

        @pl.when(i == n_chunks - 1)
        def _():
            drain_shards()

        @pl.when(z == 0)
        def _():
            for half in range(2):
                landed(hin.at[rows, pl.ds(half * d_half, d_half)], in_recv.at[half * n_chunks + i])

        @pl.when(z > 0)
        def _():
            landed(hin.at[rows, :], h_recv.at[i])

        with scope("layers"):
            layer(0, hin, rows, mid, pl.ds(0, chunk))
            layer(1, mid, pl.ds(0, chunk), hout, rows)

        @pl.when(z < PLANES - 1)
        def _():
            hop_copy(i, rows).start()

        @pl.when(z == PLANES - 1)
        def _():
            out_remote(i, rows).start()
            out_local(i, rows).start()

        return carry

    lax.fori_loop(0, n_chunks, chunk_step, 0)

    @pl.when(z < PLANES - 1)
    def _():
        each_chunk(lambda i, rows: hop_copy(i, rows).wait_send())

    @pl.when(z == PLANES - 1)
    def _():
        each_chunk(lambda i, rows: out_remote(i, rows).wait_send())
        each_chunk(lambda i, rows: out_local(i, rows).wait())

    @pl.when(z == 2)
    def _():
        each_chunk(lambda i, rows: out_remote(i, rows).wait_recv())


def _finish_kernel(
    lr, lens, w_up, w_down, g_up, g_down, y_ref,
    up_ref, down_ref, out_ref,
    up_in, down_in, up_out, down_out, y_buf, in_sem, out_sem, y_in_sem, y_out_sem, zero_sem,
):
    z = lax.axis_index("side")
    tokens = y_ref.shape[0]
    n_parts = y_in_sem.shape[0]
    part = tokens // n_parts

    def y_copy(n, out):
        rows = pl.ds(n * part, part)
        if out:
            return pltpu.make_async_copy(y_buf.at[rows, :], out_ref.at[rows, :], y_out_sem.at[n])
        return pltpu.make_async_copy(y_ref.at[rows, :], y_buf.at[rows, :], y_in_sem.at[n])

    @pl.when(z >= PLANES // 2)
    def _():
        for n in range(n_parts):
            y_copy(n, False).start()
        zeros = []
        for k, (buf, ref) in enumerate(((up_out, up_ref), (down_out, down_ref))):
            buf[0] = jnp.zeros_like(buf[0])
            for n in range(ref.shape[0]):
                zeros.append(pltpu.make_async_copy(buf.at[0], ref.at[n], zero_sem.at[k, n]))
                zeros[-1].start()
        for n in range(n_parts):
            y_copy(n, False).wait()
            rows = pl.ds(n * part, part)
            row_idx = n * part + lax.broadcasted_iota(jnp.int32, (part, 1), 0)
            y_buf[rows, :] = jnp.where(row_idx < lens[0], y_buf[rows, :], jnp.zeros((), y_buf.dtype))
            y_copy(n, True).start()
        for n in range(n_parts):
            y_copy(n, True).wait()
        for copy in zeros:
            copy.wait()

    @pl.when(z < PLANES // 2)
    def _():
        y_buf[...] = jnp.zeros_like(y_buf)
        for n in range(n_parts):
            y_copy(n, True).start()
        layers = w_up.shape[0]
        kinds = ((w_up, g_up, up_in, up_out, up_ref, 16), (w_down, g_down, down_in, down_out, down_ref, 128))

        def loads(n, k, slot):
            w, g, buf = kinds[k][:3]
            return [pltpu.make_async_copy(src.at[n], buf.at[slot, m], in_sem.at[k, slot, m])
                    for m, src in enumerate((w, g))]

        def store(n, k, slot):
            return pltpu.make_async_copy(kinds[k][3].at[slot], kinds[k][4].at[n], out_sem.at[k, slot])

        for k in range(2):
            for n in range(2):
                for copy in loads(n, k, n):
                    copy.start()

        def body(n, carry):
            slot = n % 2
            for k in range(2):
                for copy in loads(n, k, slot):
                    copy.wait()

                @pl.when(n >= 2)
                def _():
                    store(n - 2, k, slot).wait()

                src, dst, block = kinds[k][2], kinds[k][3], kinds[k][5]
                block = min(block, src.shape[2])

                def rows_body(b, c):
                    rows = pl.ds(pl.multiple_of(b * block, block), block)
                    dst[slot, rows, :] = src[slot, 0, rows, :] - lr[0] * src[slot, 1, rows, :]
                    return c
                lax.fori_loop(0, src.shape[2] // block, rows_body, 0)
                store(n, k, slot).start()

                @pl.when(n + 2 < layers)
                def _():
                    for copy in loads(n + 2, k, slot):
                        copy.start()
            return carry
        lax.fori_loop(0, layers, body, 0)
        for n in (layers - 2, layers - 1):
            for k in range(2):
                store(n, k, n % 2).wait()
        for n in range(n_parts):
            y_copy(n, True).wait()


def solution(mesh):
    tp_ways = mesh.shape["side"] // 2
    up_spec = P("side", None, "rep", None)
    down_spec = P("side", None, None, "rep")
    act_spec = P("side", "rep", None)

    def device_step(w_up, w_down, g_up, g_down, learn_rate, prompts, prompt_lens):
        w_up, w_down, g_up, g_down = w_up[0], w_down[0], g_up[0], g_down[0]
        layers, width, ff = w_up.shape
        tokens, d_half = prompts.shape[1:]
        model, hidden = width * REPS, ff * tp_ways
        chunk = min(128, tokens // 4)
        n_chunks = tokens // chunk
        dma = pltpu.SemaphoreType.DMA
        hbm = pl.BlockSpec(memory_space=pltpu.HBM)
        smem = pl.BlockSpec(memory_space=pltpu.SMEM)
        lr = learn_rate.reshape(1)
        up_shape = jax.ShapeDtypeStruct(w_up.shape, jnp.float32)
        down_shape = jax.ShapeDtypeStruct(w_down.shape, jnp.float32)
        y_shape = jax.ShapeDtypeStruct((tokens, d_half), jnp.bfloat16)
        up_in = pltpu.VMEM((2, 2, width, ff), jnp.float32)
        down_in = pltpu.VMEM((2, 2, ff, width), jnp.float32)

        y = pl.pallas_call(
            functools.partial(_pipeline_kernel, chunk=chunk, tile_n=min(512, ff), tile_m=min(512, d_half)),
            out_shape=y_shape,
            in_specs=[smem] + [hbm] * 5,
            out_specs=hbm,
            scratch_shapes=[
                pltpu.VMEM((2, model, hidden), jnp.bfloat16),
                pltpu.VMEM((2, hidden, model), jnp.bfloat16),
                pltpu.VMEM((tokens, model), jnp.bfloat16),
                pltpu.VMEM((tokens, model), jnp.bfloat16),
                pltpu.VMEM((chunk, model), jnp.bfloat16),
                pltpu.VMEM((chunk, hidden), jnp.bfloat16),
                pltpu.VMEM((layers, width, ff), jnp.bfloat16),
                pltpu.VMEM((layers, ff, width), jnp.bfloat16),
                up_in, down_in, dma((2, 2, 2)),
                dma((8,)), dma((16,)), dma((8,)), dma((8,)), dma((8,)), dma((8,)),
                dma((8,)), dma((8,)), dma((32,)), dma((32,)),
                dma((2 * n_chunks,)), dma((n_chunks,)), dma((n_chunks,)), dma((n_chunks,)),
                dma((n_chunks,)), dma((n_chunks,)), dma((n_chunks,)),
            ],
            compiler_params=pltpu.CompilerParams(
                collective_id=0, has_side_effects=True, vmem_limit_bytes=62 * 1024 * 1024),
            name="layer_pipeline",
        )(lr, w_up, w_down, g_up, g_down, prompts[0])
        new_up, new_down, out = pl.pallas_call(
            _finish_kernel,
            out_shape=(up_shape, down_shape, y_shape),
            in_specs=[smem] * 2 + [hbm] * 5,
            out_specs=(hbm, hbm, hbm),
            scratch_shapes=[
                up_in, down_in,
                pltpu.VMEM((2, width, ff), jnp.float32), pltpu.VMEM((2, ff, width), jnp.float32),
                pltpu.VMEM((tokens, d_half), jnp.bfloat16),
                dma((2, 2, 2)), dma((2, 2)), dma((4,)), dma((4,)), dma((2, layers)),
            ],
            compiler_params=pltpu.CompilerParams(vmem_limit_bytes=62 * 1024 * 1024),
            name="finish",
        )(lr, prompt_lens, w_up, w_down, g_up, g_down, y)
        return new_up[None], new_down[None], out[None]

    return jax.shard_map(
        device_step,
        mesh=mesh,
        in_specs=(up_spec, down_spec, up_spec, down_spec, P(), act_spec, P("rep")),
        out_specs=(up_spec, down_spec, act_spec),
        check_vma=False,
    )
```
